256 devices in a mesh: cell: 64 (over z, y, core), inst: 4 (over x).
Axes of the slice: x: 4, y: 4, z: 8, core: 2. Of those that a mesh axis runs over, the one named last changes fastest.
Arguments:
- fine_residual: float32 [8, 6, 524288], P('inst', None, 'cell'), may hold values from -6 to 6
- fine_map: int32 [524288], P('cell'), may hold values from 0 to 15
- routes: int32 [64, 64], P('cell'), may hold values from 0 to 63, as said below
- receive_lists: int32 [64, 192], P('cell'), may hold values from 0 to 1023
- neighbours: int32 [6, 65536], P(None, 'cell'), may hold values from 0 to 1215, as said below
- face_weights: float32 [6, 65536], P(None, 'cell'), may hold values from 0.3 to 3
- spectral_coef: float32 [65536], P('cell'), may hold values from 0.2 to 1
- diag_extra: float32 [6, 65536], P(None, 'cell'), may hold values from 0.5 to 2
Outputs:
- fine_correction: float32 [8, 6, 524288], P('inst', None, 'cell')
- coarse_correction: float32 [8, 6, 65536], P('inst', None, 'cell')
The draws below stay inside these ranges and needn't reach their ends.
Inputs may be any that keep to these rules, and one draw needn't show every extreme that they name: `routes`: in row p, the value p appears 64 - 2 * 4 times, and (p - 1) mod 64 and (p + 1) mod 64 appear 4 times each. `receive_lists`: row o, entries t * 32 to t * 32 + 31, list cells that partition o receives as halo from partition (o + d) mod 64, with d = t - 3 for t < 3 and d = t - 2 otherwise. `neighbours`: A value below 1024 is a cell of the own partition; a value x of 1024 or more is halo slot x - 1024.
All inputs are finite; a program needn't handle non-finite values.
Results may differ from the reference program's by a relative error of at most 0.0001.
Values sent between devices are 32-bit elements; how exact they have to be, the bound alone decides.
A program may use at most 64 MiB of HBM per device.

```python
import math
import jax
import jax.numpy as jnp
from jax import lax

VARS = 6
INST = 8
HB_INST = 7
NB = 6
AGG = 8
BLK = 128
RAD = 3
FB = 64
ITERS = 6
CBLK = 16
FINE = 524288
CC = 1024
COARSE = 65536
HS = 32
N_CELL = 64


def draw_routes(key, part):
    handed = FB // 16
    row_keys = jax.random.split(jax.random.fold_in(key, 17), N_CELL)

    def one_row(partition, row_key):
        slots = jnp.arange(FB, dtype=jnp.int32)
        below = jnp.mod(partition + N_CELL - 1, N_CELL)
        above = jnp.mod(partition + 1, N_CELL)
        owner_ids = jnp.where(slots < handed, below, jnp.where(slots < 2 * handed, above, partition))
        return jax.random.permutation(row_key, owner_ids)
    return jax.vmap(one_row)(jnp.arange(N_CELL, dtype=jnp.int32), row_keys).astype(jnp.int32)


def draw_neighbours(key, part):
    base = jax.random.fold_in(key, 29)
    local_key, halo_key, pick_key = jax.random.split(base, 3)
    local_ids = jax.random.randint(local_key, (NB, COARSE), 0, CC)
    halo_ids = CC + jax.random.randint(halo_key, (NB, COARSE), 0, 2 * RAD * HS)
    picked = jax.random.randint(pick_key, (NB, COARSE), 0, 5) < 4
    return jnp.where(picked, local_ids, halo_ids).astype(jnp.int32)


def touch_ends(values, rng, least, largest):
    shape = values.shape
    spot = [jax.random.randint(jax.random.fold_in(rng, axis), (), 0, shape[axis]) for axis in range(len(shape))]
    values = values.at[tuple(spot)].set(least)
    longest = shape.index(max(shape))
    spot[longest] = (spot[longest] + 1) % shape[longest]
    return values.at[tuple(spot)].set(largest)


def shard_levels(own_key, extent, cuts, low, top_value):
    def one(dim, parts):
        steps = jax.random.uniform(jax.random.fold_in(jax.random.fold_in(own_key, 6), dim), (parts,), jnp.float32, low / len(cuts), top_value / len(cuts))
        return jnp.repeat(jnp.exp(steps), extent[dim] // parts).reshape((-1,) + (1,) * (len(extent) - dim - 1))

    loudness = one(*cuts[0])
    for cut in cuts[1:]:
        loudness = loudness * one(*cut)
    return loudness


def scatter_about(rng, shape, spread, reach, pieces=(), held_as=jnp.bfloat16):
    drawn = spread * jax.random.normal(rng, shape, jnp.float32)
    if pieces:
        drawn = drawn * shard_levels(rng, shape, pieces, -0.22, 0.18)
    return jnp.clip(drawn, -reach, reach).astype(held_as)


def setup_inputs(seed: int = 0) -> dict:
    key_of = jax.random.split(jax.random.key(seed), 9)
    return {
        "fine_residual": scatter_about(key_of[0], (INST, VARS, FINE), 1.0, 6.0, ((0, 4), (2, 64)), jnp.float32),
        "fine_map": touch_ends(jax.random.randint(key_of[1], (FINE,), 0, BLK // AGG), jax.random.fold_in(key_of[1], 1), 0, (BLK // AGG) - 1).astype(jnp.int32),
        "routes": draw_routes(jax.random.fold_in(key_of[8], 71), 0),
        "receive_lists": touch_ends(jax.random.randint(key_of[3], (N_CELL, 2 * RAD * HS), 0, CC), jax.random.fold_in(key_of[3], 1), 0, CC - 1).astype(jnp.int32),
        "neighbours": draw_neighbours(jax.random.fold_in(key_of[8], 71), 0),
        "face_weights": jnp.clip(jnp.exp(math.log(3.0) - 2.3025851 * jax.random.uniform(key_of[5], (NB, COARSE), jnp.float32) ** shard_levels(key_of[5], (NB, COARSE), ((1, 64),), -0.2, 0.2)), 0.3, 3.0),
        "spectral_coef": jnp.clip(jnp.exp(math.log(1.0) - 1.609438 * jax.random.uniform(key_of[6], (COARSE,), jnp.float32) ** shard_levels(key_of[6], (COARSE,), ((0, 64),), -0.2, 0.2)), 0.2, 1.0),
        "diag_extra": jnp.clip(jnp.exp(math.log(2.0) - 1.3862944 * jax.random.uniform(key_of[7], (VARS, COARSE), jnp.float32) ** shard_levels(key_of[7], (VARS, COARSE), ((1, 64),), -0.2, 0.2)), 0.5, 2.0),
    }


exact_precision = lax.Precision.HIGHEST


def spectral_matrix():
    row_ids = jnp.arange(INST)[:, None]
    col_ids = jnp.arange(INST)[None, :]
    distance = row_ids - col_ids
    usable = (row_ids < HB_INST) & (col_ids < HB_INST) & (distance != 0)
    parity = 1.0 - 2.0 * jnp.mod(distance, 2).astype(jnp.float32)
    denominator = jnp.sin(jnp.pi * jnp.where(usable, distance, 1).astype(jnp.float32) / HB_INST)
    return jnp.where(usable, 0.5 * parity / denominator, 0.0).astype(jnp.float32)


def reference(fine_residual, fine_map, routes, receive_lists, neighbours, face_weights, spectral_coef, diag_extra):
    source = jnp.arange(N_CELL, dtype=jnp.int32)[:, None]
    relative = jnp.mod(routes - source, N_CELL)
    category = jnp.where(relative == 1, 0, jnp.where(relative == 0, 1, 2)).astype(jnp.int32)
    block_order = jnp.argsort(category, axis=1, stable=True).astype(jnp.int32)
    position = jnp.argsort(block_order, axis=1, stable=True).astype(jnp.int32)
    block_base = routes * CC + position * CBLK
    coarse_of_fine = (block_base[:, :, None] + fine_map.reshape(N_CELL, FB, BLK)).reshape(-1).astype(jnp.int32)
    flat_fine = fine_residual.reshape(INST * VARS, FINE).T
    coarse_residual = jax.ops.segment_sum(flat_fine, coarse_of_fine, num_segments=COARSE).T.reshape(INST, VARS, COARSE)
    inst_ids = jnp.arange(INST)
    coarse_residual = jnp.where((inst_ids < HB_INST)[:, None, None], coarse_residual, jnp.float32(0.0))
    owners = (jnp.arange(COARSE, dtype=jnp.int32) // CC)[None, :]
    is_local = neighbours < CC
    halo_slot = jnp.maximum(neighbours - CC, 0)
    peer_slot = halo_slot // HS
    offset = jnp.where(peer_slot < RAD, peer_slot - RAD, peer_slot - RAD + 1)
    sender = jnp.mod(owners + offset, N_CELL)
    remote_index = receive_lists[jnp.broadcast_to(owners, neighbours.shape), halo_slot]
    neighbour_ids = jnp.where(is_local, owners * CC + neighbours, sender * CC + remote_index).astype(jnp.int32)
    diagonal = jnp.sum(face_weights, axis=0)[None, :] + 3.0 * spectral_coef[None, :] + diag_extra
    spectral = spectral_matrix()
    correction = coarse_residual / diagonal[None]
    for sweep in range(ITERS):
        neighbour_sum = jnp.zeros_like(correction)
        for slot_index in range(NB):
            neighbour_sum = neighbour_sum + face_weights[slot_index][None, None, :] * jnp.take(correction, neighbour_ids[slot_index], axis=2)
        coupling = jnp.einsum("nm,mvc->nvc", spectral, correction, precision=exact_precision)
        correction = (coarse_residual + neighbour_sum - spectral_coef[None, None, :] * coupling) / diagonal[None]
    fine_correction = jnp.take(correction, coarse_of_fine, axis=2)
    return fine_correction, correction
```

```python
import functools
import math

import jax
import jax.numpy as jnp
from jax import lax
from jax.experimental import pallas as pl
from jax.experimental.pallas import tpu as pltpu
from jax.sharding import PartitionSpec as P

INST = 8
HB_INST = 7
VARS = 6
NB = 6
BLK = 128
CB = 16
RAD = 3
HS = 32
ITERS = 6
PEERS = 2 * RAD
OFFSETS = [t - RAD if t < RAD else t - RAD + 1 for t in range(PEERS)]
SWEEPERS = 3
ROWS = 16
SEND = 256
MESH = pl.DeviceIdType.MESH
F32 = jnp.float32
BF16 = jnp.bfloat16
T_Q, T_R, T_H, T_L = 0, 96, 192, 288
T_S, T_D, T_END = 384, 432, 480


def spectral_value(distance):
    if distance == 0:
        return 0.0
    sign = -1.0 if distance % 2 else 1.0
    return 0.5 * sign / math.sin(math.pi * distance / HB_INST)


def split2(x):
    hi = x.astype(BF16)
    return hi, (x - hi.astype(F32)).astype(BF16)


def split3(x):
    hi = x.astype(BF16)
    rest = x - hi.astype(F32)
    mid = rest.astype(BF16)
    return hi, mid, (rest - mid.astype(F32)).astype(BF16)


def dot(a, b):
    return lax.dot_general(a, b, (((1,), (0,)), ((), ())), preferred_element_type=F32)


def dot_t(a, b):
    return lax.dot_general(a, b, (((1,), (1,)), ((), ())), preferred_element_type=F32)


def kernel(
    n_cell,
    fr, fm, rt, rl, nb, fw, sc, de,
    coarse_o, blocks_o,
    fr_v, fm_v, rt_s, rl_v, nb_v, fw_v, sc_v, de_v,
    inv_v, pos_v, perm, perm_t, yu,
    ysend, rx, rx0, rx7, lsend, lrx,
    table, stable, sel, wh, wl, coef,
    r_v, sg_v, di_v, base_v, x_v, xh_v,
    xsend, halo, xf, gx, gx0, gx7,
    in_sem,
    l_ss, l_rs, r_ss, r_rs, h_ss, h_rs, f_ss, f_rs,
):
    cell = lax.axis_index("cell")
    inst = lax.axis_index("inst")
    blocks = fm_v.shape[0]
    handed = blocks // 16
    cc = blocks * CB
    n_inst = 4

    def at_cell(d):
        return lax.rem(cell + (d + n_cell), n_cell)

    def copy_in(i, src, dst):
        c = pltpu.make_async_copy(src, dst, in_sem.at[i])
        c.start()
        return c

    c_rt = copy_in(0, rt, rt_s)
    c_fr = copy_in(1, fr, fr_v)
    c_fm = copy_in(2, fm, fm_v)
    c_rl = copy_in(3, rl, rl_v)
    c_nb = copy_in(4, nb, nb_v)
    c_fw = copy_in(5, fw, fw_v)
    c_sc = copy_in(6, sc, sc_v)
    c_de = copy_in(7, de, de_v)

    barrier = pltpu.get_barrier_semaphore()
    partners = 0
    for d in OFFSETS:
        pl.semaphore_signal(barrier, inc=1, device_id={"cell": at_cell(d), "inst": inst}, device_id_type=MESH)
        partners += 1
    for d in (0, -1, 1):
        for j in range(1, n_inst):
            pl.semaphore_signal(
                barrier, inc=1,
                device_id={"cell": at_cell(d), "inst": lax.rem(inst + j, n_inst)},
                device_id_type=MESH,
            )
            partners += 1

    c_rt.wait()
    group = lax.broadcasted_iota(jnp.int32, (8, BLK), 0) * 8 + lax.broadcasted_iota(jnp.int32, (8, BLK), 1) // CB

    def find(step, carry):
        c0, c1, c2, inv, fwd = carry
        for u in range(8):
            b = step * 8 + u
            rel = lax.rem(rt_s[0, b] - cell + n_cell, n_cell)
            is0 = rel == 1
            is1 = rel == 0
            pos = jnp.where(is0, c0, jnp.where(is1, c1, c2))
            c0 = c0 + jnp.where(is0, 1, 0)
            c1 = c1 + jnp.where(is1, 1, 0)
            c2 = c2 + jnp.where(is0 | is1, 0, 1)
            inv = jnp.where(group == pos, b, inv)
            fwd = jnp.where(group == b, pos, fwd)
        return c0, c1, c2, inv, fwd

    zero8 = jnp.zeros((8, BLK), jnp.int32)
    init = (jnp.int32(0), jnp.int32(handed), jnp.int32(blocks - handed), zero8, zero8)
    found = lax.fori_loop(0, blocks // 8, find, init)
    within = lax.rem(lax.broadcasted_iota(jnp.int32, (8, BLK), 1), CB)
    inv_v[...] = found[3] * CB + within
    pos_v[...] = found[4] * CB + within

    c_nb.wait()
    c_fw.wait()
    c_sc.wait()
    c_de.wait()
    ids = [jnp.broadcast_to(nb_v[s : s + 1, :], (8, cc)) for s in range(NB)]
    face = [jnp.broadcast_to(fw_v[s : s + 1, :], (8, cc)) for s in range(NB)]
    total = face[0]
    for s in range(1, NB):
        total = total + face[s]
    for s in range(NB):
        for o in range(s + 1, NB):
            same = ids[s] == ids[o]
            face[s] = face[s] + jnp.where(same, face[o], 0.0)
            ids[o] = jnp.where(same, 2047, ids[o])

    def twice(x):
        return jnp.concatenate([x, x], axis=0)

    for s in range(NB):
        rows = pl.ds(16 * s, 16)
        table[pl.ds(T_Q + 16 * s, 16), :] = twice((ids[s] // 256).astype(F32)).astype(BF16)
        table[pl.ds(T_R + 16 * s, 16), :] = twice((ids[s] % 256).astype(F32)).astype(BF16)
        hi, lo = split2(twice(face[s]))
        table[pl.ds(T_H + 16 * s, 16), :] = hi
        table[pl.ds(T_L + 16 * s, 16), :] = lo
    sig = jnp.broadcast_to(sc_v[0:1, :], (8, cc))
    pair = [
        jnp.where(inst == 0, de_v[v : v + 1, :], jnp.where(inst == 1, de_v[2 + v : 3 + v, :], de_v[4 + v : 5 + v, :]))
        for v in range(2)
    ]
    odd = lax.rem(lax.broadcasted_iota(jnp.int32, (8, cc), 0), 4) >= 2
    diag = total + 3.0 * sig + jnp.where(odd, jnp.broadcast_to(pair[1], (8, cc)), jnp.broadcast_to(pair[0], (8, cc)))
    for k, part in enumerate(split3(twice(sig))):
        table[pl.ds(T_S + 16 * k, 16), :] = part
    for k, part in enumerate(split3(twice(diag))):
        table[pl.ds(T_D + 16 * k, 16), :] = part
    sg_v[:, SEND:] = twice(sig)
    di_v[:, SEND:] = twice(1.0 / diag)

    row = lax.broadcasted_iota(jnp.int32, (ROWS, BLK), 0)
    row_n = 2 * (row // 4) + row % 2
    row_v = (row % 4) // 2
    live = [p for p in range(ROWS) if 2 * (p // 4) + p % 2 < HB_INST]
    for slot, p in enumerate(live):
        n, v = 2 * (p // 4) + p % 2, (p % 4) // 2
        value = jnp.zeros((ROWS, BLK), F32)
        for m in range(HB_INST):
            value = jnp.where((row_n == m) & (row_v == v), spectral_value(m - n), value)
        coef[slot] = value

    row16 = lax.broadcasted_iota(jnp.int32, (16, BLK), 0).astype(F32).astype(BF16)

    def permutation(src, dst):
        def one(tile, _):
            line = jnp.broadcast_to(src[pl.ds(tile, 1), :], (16, BLK))
            lanes = pl.ds(pl.multiple_of(tile * BLK, BLK), BLK)
            high = (line // 256).astype(F32).astype(BF16)
            low = lax.rem(line, 256).astype(F32).astype(BF16)
            for kt in range(cc // 256):
                at = jnp.where(high == jnp.asarray(kt, BF16), low, jnp.full_like(low, -1.0))
                for j in range(16):
                    hit = at == row16 + jnp.asarray(16.0 * j, BF16)
                    dst[256 * kt + 16 * j : 256 * kt + 16 * j + 16, lanes] = jnp.where(
                        hit, jnp.ones((16, BLK), BF16), jnp.zeros((16, BLK), BF16)
                    )
            return 0

        lax.fori_loop(0, cc // BLK, one, 0)

    permutation(inv_v, perm)

    c_fr.wait()
    c_fm.wait()
    kept = 2 * inst + 1 < HB_INST
    rows_of = lax.rem(lax.broadcasted_iota(jnp.int32, (BLK, BLK), 0), CB)
    block_of = lax.broadcasted_iota(jnp.int32, (16, BLK), 0) // 2 == lax.broadcasted_iota(jnp.int32, (16, BLK), 1) // CB
    drop = (lax.rem(lax.broadcasted_iota(jnp.int32, (2, BLK), 0), 2) == 0) | kept

    def restrict(tile, _):
        maps = [jnp.broadcast_to(fm_v[pl.ds(tile * 8 + e, 1), :], (CB, BLK)) for e in range(8)]
        onehot = jnp.where(rows_of == jnp.concatenate(maps, axis=0), 1.0, 0.0).astype(BF16)
        rows = pl.ds(pl.multiple_of(tile * 16, 16), 16)
        lanes = pl.ds(pl.multiple_of(tile * BLK, BLK), BLK)
        his, los = [], []
        for v in range(VARS):
            hi, lo = split2(fr_v[v, rows, :])
            his.append(hi)
            los.append(lo)
        got = dot_t(jnp.concatenate(his + los, axis=0), onehot)
        for v in range(VARS):
            both = jnp.where(block_of, got[16 * v : 16 * v + 16] + got[96 + 16 * v : 112 + 16 * v], 0.0)
            half = both[0:8] + both[8:16]
            half = half[0:4] + half[4:8]
            yu[v // 2, 2 * (v % 2) : 2 * (v % 2) + 2, lanes] = jnp.where(drop, half[0:2] + half[2:4], 0.0)
        return 0

    lax.fori_loop(0, cc // BLK, restrict, 0)
    terms = split3(jnp.concatenate([yu[0], yu[1], yu[2], yu[2]], axis=0))
    terms = jnp.concatenate(terms, axis=0)
    for nt in (0, cc // 256 - 1, *range(1, cc // 256 - 1)):
        got = dot(terms, perm[:, 256 * nt : 256 * nt + 256])
        got = got[0:16] + got[16:32] + got[32:48]
        for g in range(SWEEPERS):
            ysend[g, :, 256 * nt : 256 * nt + 256] = got[4 * g : 4 * g + 4, :]

    c_rl.wait()
    lsend[...] = jnp.zeros_like(lsend)
    lsend[:, : PEERS * HS] = rl_v[...]

    pl.semaphore_wait(barrier, partners)

    def list_copy(t, target_cell):
        return pltpu.make_async_remote_copy(
            src_ref=lsend, dst_ref=lrx.at[t], send_sem=l_ss.at[t], recv_sem=l_rs.at[t],
            device_id={"cell": target_cell, "inst": inst}, device_id_type=MESH,
        )

    def rest_copy(g, kind, src):
        lanes = (pl.ds(0, cc), pl.ds(0, BLK), pl.ds(cc - BLK, BLK))[kind]
        dst = (rx, rx0, rx7)[kind]
        return pltpu.make_async_remote_copy(
            src_ref=ysend.at[g, :, lanes], dst_ref=dst.at[src], send_sem=r_ss.at[kind, g], recv_sem=r_rs.at[kind, src],
            device_id={"cell": at_cell((0, 1, -1)[kind]), "inst": g}, device_id_type=MESH,
        )

    def halo_copy(k, t):
        return pltpu.make_async_remote_copy(
            src_ref=xsend.at[k, t // 4], dst_ref=halo.at[k, t], send_sem=h_ss.at[k, t], recv_sem=h_rs.at[k, t],
            device_id={"cell": at_cell(-OFFSETS[t]), "inst": inst}, device_id_type=MESH,
        )

    def back_copy(g, kind, src):
        lanes = (pl.ds(0, cc), pl.ds(0, BLK), pl.ds(cc - BLK, BLK))[kind]
        dst = (gx, gx0, gx7)[kind]
        return pltpu.make_async_remote_copy(
            src_ref=xf.at[g, :, lanes], dst_ref=dst.at[src], send_sem=f_ss.at[kind, g], recv_sem=f_rs.at[kind, src],
            device_id={"cell": at_cell((0, -1, 1)[kind]), "inst": g}, device_id_type=MESH,
        )

    sweeping = inst < SWEEPERS

    @pl.when(sweeping)
    def _():
        for t in range(PEERS):
            list_copy(t, at_cell(OFFSETS[t])).start()

    for kind in (1, 2):
        for g in range(SWEEPERS):
            rest_copy(g, kind, inst).start()
    for g in range(SWEEPERS):
        @pl.when(inst != g)
        def _():
            rest_copy(g, 0, inst).start()

        @pl.when(inst == g)
        def _():
            rx[g] = ysend[g]

    quarter = lax.broadcasted_iota(jnp.int32, (ROWS, BLK), 1) // HS

    def build(src, lane_tiles, first_tile):
        def one(m, _):
            lt, kt = m // 5, lax.rem(m, 5)
            s_lanes = pl.ds(pl.multiple_of(lt * BLK, BLK), BLK)
            d_lanes = pl.ds(pl.multiple_of((lt + first_tile) * BLK, BLK), BLK)
            kf = kt.astype(F32).astype(BF16)
            at = []
            for s in range(NB):
                q = src[pl.ds(T_Q + 16 * s, 16), s_lanes]
                r = src[pl.ds(T_R + 16 * s, 16), s_lanes]
                at.append(jnp.where(q == kf, r, jnp.full_like(r, -1.0)))
            hs = [src[pl.ds(T_H + 16 * s, 16), s_lanes] for s in range(NB)]
            ls = [src[pl.ds(T_L + 16 * s, 16), s_lanes] for s in range(NB)]
            for j in range(16):
                here = row16 + jnp.asarray(16.0 * j, BF16)
                h = jnp.zeros((16, BLK), BF16)
                low = jnp.zeros((16, BLK), BF16)
                for s in range(NB):
                    hit = at[s] == here
                    h = jnp.where(hit, hs[s], h)
                    low = jnp.where(hit, ls[s], low)
                k_rows = pl.ds(pl.multiple_of(kt * 256 + 16 * j, 16), 16)
                wh[k_rows, d_lanes] = h
                wl[k_rows, d_lanes] = low
            return 0

        lax.fori_loop(0, lane_tiles * 5, one, 0)

    def local_part(x_all):
        own_hi, own_lo = split2(x_all[:, SEND:])
        xh_v[0:16, :] = own_hi
        xh_v[16:32, :] = own_lo
        x_v[...] = x_all
        for nt in range((SEND + cc) // 256):
            lanes = pl.ds(256 * nt, 256)
            a = dot(xh_v[...], wh[0:cc, lanes])
            b = dot(xh_v[0:16, :], wl[0:cc, lanes])
            halves = []
            for e in range(2):
                part = pl.ds(256 * nt + 128 * e, 128)
                acc = jnp.zeros((ROWS, BLK), F32)
                for slot, p in enumerate(live):
                    acc = acc + coef[slot] * jnp.broadcast_to(x_v[p : p + 1, part], (ROWS, BLK))
                halves.append(acc)
            sx = jnp.concatenate(halves, axis=1)
            base_v[:, lanes] = r_v[:, lanes] - sg_v[:, lanes] * sx + (a[0:16] + a[16:32] + b)

    def halo_rows(k):
        for t in range(PEERS):
            halo_copy(k, t).wait_recv()
        first = halo[k, 0]
        for t in range(1, 4):
            first = jnp.where(quarter == t, halo[k, t], first)
        second = jnp.where(quarter == 0, halo[k, 4], jnp.where(quarter == 1, halo[k, 5], 0.0))
        hi, lo = split2(jnp.concatenate([first, second], axis=1))
        return jnp.concatenate([hi, lo], axis=0)

    def with_halo(rows, lanes):
        a = dot(rows, wh[cc : cc + 256, lanes])
        b = dot(rows[0:16], wl[cc : cc + 256, lanes])
        return (base_v[:, lanes] + (a[0:16] + a[16:32] + b)) * di_v[:, lanes]

    def send_halo(k, x_send):
        xsend[k, 0] = x_send[:, 0:BLK]
        xsend[k, 1] = x_send[:, BLK:SEND]
        for t in range(PEERS):
            halo_copy(k, t).start()

    @pl.when(sweeping)
    def _():
        build(table, cc // BLK, SEND // BLK)
        permutation(pos_v, perm_t)
        for t in range(PEERS):
            list_copy(t, at_cell(OFFSETS[t])).wait_recv()
        lane_slot = lax.broadcasted_iota(jnp.int32, (1, SEND), 1) // HS
        wanted = jnp.full((1, SEND), 4096, jnp.int32)
        for t in range(PEERS):
            wanted = jnp.where(lane_slot == t, lrx[t], wanted)
        for kt in range(cc // 256):
            rows256 = lax.broadcasted_iota(jnp.int32, (256, SEND), 0) + 256 * kt
            sel[256 * kt : 256 * kt + 256, :] = jnp.where(rows256 == wanted, 1.0, 0.0).astype(BF16)
        taken = dot(table[...], sel[...])
        stable[...] = taken[0:T_S].astype(BF16)
        used = lane_slot < PEERS
        sg_v[:, 0:SEND] = taken[T_S : T_S + 16] + taken[T_S + 16 : T_S + 32] + taken[T_S + 32 : T_S + 48]
        d_send = taken[T_D : T_D + 16] + taken[T_D + 16 : T_D + 32] + taken[T_D + 32 : T_D + 48]
        di_v[:, 0:SEND] = 1.0 / jnp.where(used, d_send, 1.0)
        build(stable, SEND // BLK, 0)

        for src in range(n_inst):
            for kind in (1, 2):
                rest_copy(0, kind, src).wait_recv()

            @pl.when(inst != src)
            def _():
                rest_copy(0, 0, src).wait_recv()

        lane = lax.broadcasted_iota(jnp.int32, (ROWS, BLK), 1)
        mine = jnp.concatenate([rx[src] for src in range(n_inst)], axis=0)
        low = jnp.concatenate([rx0[src] for src in range(n_inst)], axis=0)
        high = jnp.concatenate([rx7[src] for src in range(n_inst)], axis=0)
        edge = handed * CB
        rest = jnp.concatenate(
            [
                jnp.where(lane < edge, low, mine[:, 0:BLK]),
                mine[:, BLK : cc - BLK],
                jnp.where(lane >= BLK - edge, high, mine[:, cc - BLK :]),
            ],
            axis=1,
        )
        parts = dot(jnp.concatenate(split3(rest), axis=0), sel[...])
        r_send = parts[0:16] + parts[16:32] + parts[32:48]
        x_send = r_send * di_v[:, 0:SEND]
        send_halo(0, x_send)
        r_v[:, 0:SEND] = r_send
        r_v[:, SEND:] = rest
        local_part(jnp.concatenate([x_send, rest * di_v[:, SEND:]], axis=1))

        def sweep(k, _):
            rows = halo_rows(k)
            x_send = with_halo(rows, pl.ds(0, SEND))
            send_halo(k + 1, x_send)
            parts = [x_send]
            for nt in range(cc // 256):
                parts.append(with_halo(rows, pl.ds(SEND + 256 * nt, 256)))
            local_part(jnp.concatenate(parts, axis=1))
            return 0

        lax.fori_loop(0, ITERS - 1, sweep, 0)
        rows = halo_rows(ITERS - 1)
        for nt in (0, cc // 256 - 1, *range(1, cc // 256 - 1)):
            out = with_halo(rows, pl.ds(SEND + 256 * nt, 256))
            for g in range(n_inst):
                xf[g, :, 256 * nt : 256 * nt + 256] = out[4 * g : 4 * g + 4, :]
            if nt == cc // 256 - 1:
                for kind in (1, 2):
                    for g in range(n_inst):
                        back_copy(g, kind, inst).start()
        for g in range(n_inst):
            @pl.when(inst != g)
            def _():
                back_copy(g, 0, inst).start()

            @pl.when(inst == g)
            def _():
                if g < SWEEPERS:
                    gx[g] = xf[g]

    @pl.when(jnp.logical_not(sweeping))
    def _():
        permutation(pos_v, perm_t)

    lane4 = lax.broadcasted_iota(jnp.int32, (4, BLK), 1)
    edge = handed * CB
    placed = []
    for src in range(SWEEPERS):
        for kind in (1, 2):
            back_copy(0, kind, src).wait_recv()

        @pl.when(inst != src)
        def _():
            back_copy(0, 0, src).wait_recv()

        own = gx[src]
        first = jnp.where(lane4 < edge, gx0[src], own[:, 0:BLK])
        last = jnp.where(lane4 >= BLK - edge, gx7[src], own[:, cc - BLK :])
        coarse_o[src] = own
        placed.append(jnp.concatenate([first, own[:, BLK : cc - BLK], last], axis=1))
    terms = jnp.concatenate(split3(jnp.concatenate(placed + placed[2:], axis=0)), axis=0)
    for nt in range(cc // 256):
        got = dot(terms, perm_t[:, 256 * nt : 256 * nt + 256])
        got = got[0:16] + got[16:32] + got[32:48]
        for g in range(SWEEPERS):
            blocks_o[g, :, 256 * nt : 256 * nt + 256] = got[4 * g : 4 * g + 4, :]

    for kind in (1, 2):
        for g in range(SWEEPERS):
            rest_copy(g, kind, inst).wait_send()
    for g in range(SWEEPERS):
        @pl.when(inst != g)
        def _():
            rest_copy(g, 0, inst).wait_send()

    @pl.when(sweeping)
    def _():
        for t in range(PEERS):
            list_copy(t, at_cell(OFFSETS[t])).wait_send()
            for k in range(ITERS):
                halo_copy(k, t).wait_send()
        for g in range(n_inst):
            for kind in (1, 2):
                back_copy(g, kind, inst).wait_send()

            @pl.when(inst != g)
            def _():
                back_copy(g, 0, inst).wait_send()


def prolong(fm, coarse, blocks_x, fine_o, coarse_o):
    for v in range(VARS):
        coarse_o[v] = coarse[v // 2, 2 * (v % 2) : 2 * (v % 2) + 2, :]
    for tile in range(blocks_x.shape[2] // BLK):
        lanes = pl.ds(tile * BLK, BLK)
        for half in range(2):
            maps = [
                jnp.broadcast_to(fm[tile * 8 + 4 * half + e : tile * 8 + 4 * half + e + 1, :], (2, BLK)) + (4 * half + e) * CB
                for e in range(4)
            ]
            index = jnp.concatenate(maps, axis=0)
            rows = pl.ds(16 * tile + 8 * half, 8)
            for v in range(VARS):
                x = blocks_x[v // 2, 2 * (v % 2) : 2 * (v % 2) + 2, lanes]
                x = jnp.concatenate([x, x, x, x], axis=0)
                fine_o[v, rows, :] = jnp.take_along_axis(x, index, axis=1, mode="promise_in_bounds")


def body(n_cell, fine_residual, fine_map, routes, receive_lists, neighbours, face_weights, spectral_coef, diag_extra):
    inst_dev, var_count, fine_dev = fine_residual.shape
    blocks = fine_dev // BLK
    cc = blocks * CB
    lanes = SEND + cc
    vmem = pltpu.VMEM
    dma = pltpu.SemaphoreType.DMA
    any_spec = pl.BlockSpec(memory_space=pl.ANY)
    out_spec = pl.BlockSpec(memory_space=pltpu.VMEM)
    fine_rows = fine_residual.reshape(inst_dev, var_count, blocks, BLK).transpose(1, 2, 0, 3)
    fine_rows = fine_rows.reshape(var_count, blocks * inst_dev, BLK)
    cells_map = fine_map.reshape(blocks, BLK)
    coarse, in_blocks = pl.pallas_call(
        functools.partial(kernel, n_cell),
        out_shape=(
            jax.ShapeDtypeStruct((SWEEPERS, 4, cc), F32),
            jax.ShapeDtypeStruct((SWEEPERS, 4, cc), F32),
        ),
        in_specs=[any_spec] * 8,
        out_specs=(out_spec, out_spec),
        scratch_shapes=[
            vmem(fine_rows.shape, F32),
            vmem((blocks, BLK), jnp.int32),
            pltpu.SMEM((1, blocks), jnp.int32),
            vmem((1, PEERS * HS), jnp.int32),
            vmem((NB, cc), jnp.int32),
            vmem((NB, cc), F32),
            vmem((1, cc), F32),
            vmem((VARS, cc), F32),
            vmem((8, BLK), jnp.int32),
            vmem((8, BLK), jnp.int32),
            vmem((cc, cc), BF16),
            vmem((cc, cc), BF16),
            vmem((SWEEPERS, 4, cc), F32),
            vmem((SWEEPERS, 4, cc), F32),
            vmem((4, 4, cc), F32),
            vmem((4, 4, BLK), F32),
            vmem((4, 4, BLK), F32),
            vmem((1, SEND), jnp.int32),
            vmem((PEERS, 1, SEND), jnp.int32),
            vmem((T_END, cc), BF16),
            vmem((T_S, SEND), BF16),
            vmem((cc, SEND), BF16),
            vmem((cc + 256, lanes), BF16),
            vmem((cc + 256, lanes), BF16),
            vmem((2 * HB_INST, ROWS, BLK), F32),
            vmem((ROWS, lanes), F32),
            vmem((ROWS, lanes), F32),
            vmem((ROWS, lanes), F32),
            vmem((ROWS, lanes), F32),
            vmem((ROWS, lanes), F32),
            vmem((2 * ROWS, cc), BF16),
            vmem((ITERS, 2, ROWS, BLK), F32),
            vmem((ITERS, PEERS, ROWS, BLK), F32),
            vmem((4, 4, cc), F32),
            vmem((SWEEPERS, 4, cc), F32),
            vmem((SWEEPERS, 4, BLK), F32),
            vmem((SWEEPERS, 4, BLK), F32),
            dma((8,)),
            dma((PEERS,)),
            dma((PEERS,)),
            dma((3, SWEEPERS)),
            dma((3, 4)),
            dma((ITERS, PEERS)),
            dma((ITERS, PEERS)),
            dma((3, 4)),
            dma((3, SWEEPERS)),
        ],
        compiler_params=pltpu.CompilerParams(collective_id=0, has_side_effects=True),
        name="multigrid",
    )(
        fine_rows,
        cells_map,
        routes,
        receive_lists,
        neighbours,
        face_weights,
        spectral_coef.reshape(1, cc),
        diag_extra,
    )
    fine, coarse = pl.pallas_call(
        prolong,
        out_shape=(
            jax.ShapeDtypeStruct(fine_rows.shape, F32),
            jax.ShapeDtypeStruct((var_count, inst_dev, cc), F32),
        ),
        in_specs=[out_spec] * 3,
        out_specs=(out_spec, out_spec),
        name="prolong",
    )(cells_map, coarse, in_blocks)
    fine = fine.reshape(var_count, blocks, inst_dev, BLK).transpose(2, 0, 1, 3).reshape(inst_dev, var_count, fine_dev)
    return fine, coarse.transpose(1, 0, 2)


def solution(mesh):
    in_specs = (
        P("inst", None, "cell"),
        P("cell"),
        P("cell", None),
        P("cell", None),
        P(None, "cell"),
        P(None, "cell"),
        P("cell"),
        P(None, "cell"),
    )
    out_specs = (P("inst", None, "cell"), P("inst", None, "cell"))
    return jax.shard_map(
        functools.partial(body, mesh.shape["cell"]), mesh=mesh, in_specs=in_specs, out_specs=out_specs, check_vma=False
    )
```

```python
import functools
import math

import jax
import jax.numpy as jnp
from jax import lax
from jax.experimental import pallas as pl
from jax.experimental.pallas import tpu as pltpu
from jax.sharding import PartitionSpec as P

INST = 8
HB_INST = 7
VARS = 6
NB = 6
BLK = 128
CB = 16
RAD = 3
HS = 32
ITERS = 6
PEERS = 2 * RAD
OFFSETS = [t - RAD if t < RAD else t - RAD + 1 for t in range(PEERS)]
SWEEPERS = 3
ROWS = 16
SEND = 256
MESH = pl.DeviceIdType.MESH
F32 = jnp.float32
BF16 = jnp.bfloat16
T_Q, T_R, T_H, T_L = 0, 96, 192, 288
T_S, T_D, T_END = 384, 432, 480


def spectral_value(distance):
    if distance == 0:
        return 0.0
    sign = -1.0 if distance % 2 else 1.0
    return 0.5 * sign / math.sin(math.pi * distance / HB_INST)


def split2(x):
    hi = x.astype(BF16)
    return hi, (x - hi.astype(F32)).astype(BF16)


def split3(x):
    hi = x.astype(BF16)
    rest = x - hi.astype(F32)
    mid = rest.astype(BF16)
    return hi, mid, (rest - mid.astype(F32)).astype(BF16)


def dot(a, b):
    return lax.dot_general(a, b, (((1,), (0,)), ((), ())), preferred_element_type=F32)


def dot_t(a, b):
    return lax.dot_general(a, b, (((1,), (1,)), ((), ())), preferred_element_type=F32)


def kernel(
    n_cell,
    fr, fm, rt, rl, nb, fw, sc, de,
    coarse_o, blocks_o,
    fr_v, fm_v, rt_s, rl_v, nb_v, fw_v, sc_v, de_v,
    inv_v, pos_v, perm, perm_t, yu,
    ysend, rx, rxe, lsend, lrx,
    table, stable, sel, wh, wl, coef,
    r_v, sg_v, di_v, base_v, x_v, xh_v,
    xsend, halo, xf, gx, gxe,
    in_sem, out_sem, list_sem, rest_sem, halo_sem, back_sem,
):
    cell = lax.axis_index("cell")
    inst = lax.axis_index("inst")
    blocks = fm_v.shape[0]
    handed = blocks // 16
    cc = blocks * CB
    n_inst = 4

    def at_cell(d):
        return lax.rem(cell + (d + n_cell), n_cell)

    def copy_in(i, src, dst):
        c = pltpu.make_async_copy(src, dst, in_sem.at[i])
        c.start()
        return c

    c_rt = copy_in(0, rt, rt_s)
    c_fr = copy_in(1, fr, fr_v)
    c_fm = copy_in(2, fm, fm_v)
    c_rl = copy_in(3, rl, rl_v)
    c_nb = copy_in(4, nb, nb_v)
    c_fw = copy_in(5, fw, fw_v)
    c_sc = copy_in(6, sc, sc_v)
    c_de = copy_in(7, de, de_v)

    barrier = pltpu.get_barrier_semaphore()
    partners = 0
    for d in OFFSETS:
        pl.semaphore_signal(barrier, inc=1, device_id={"cell": at_cell(d), "inst": inst}, device_id_type=MESH)
        partners += 1
    for d in (0, -1, 1):
        for j in range(1, n_inst):
            pl.semaphore_signal(
                barrier, inc=1,
                device_id={"cell": at_cell(d), "inst": lax.rem(inst + j, n_inst)},
                device_id_type=MESH,
            )
            partners += 1

    c_rt.wait()
    group = lax.broadcasted_iota(jnp.int32, (8, BLK), 0) * 8 + lax.broadcasted_iota(jnp.int32, (8, BLK), 1) // CB

    above = at_cell(1)

    def find(step, carry):
        c0, c1, inv, fwd = carry
        for u in range(8):
            b = step * 8 + u
            route = rt_s[0, b]
            is0 = route == above
            is1 = route == cell
            pos = jnp.where(is1, c1, jnp.where(is0, c0, blocks + b - c0 - c1))
            c0 = c0 + jnp.where(is0, 1, 0)
            c1 = c1 + jnp.where(is1, 1, 0)
            inv = jnp.where(group == pos, b, inv)
            fwd = jnp.where(group == b, pos, fwd)
        return c0, c1, inv, fwd

    zero8 = jnp.zeros((8, BLK), jnp.int32)
    found = lax.fori_loop(0, blocks // 8, find, (jnp.int32(0), jnp.int32(handed), zero8, zero8))
    within = lax.rem(lax.broadcasted_iota(jnp.int32, (8, BLK), 1), CB)
    inv_v[...] = found[2] * CB + within
    pos_v[...] = found[3] * CB + within

    row16 = lax.broadcasted_iota(jnp.int32, (16, BLK), 0).astype(F32).astype(BF16)

    def permutation_tile(src, dst, tile):
        line = jnp.broadcast_to(src[pl.ds(tile, 1), :], (16, BLK))
        lanes = pl.ds(pl.multiple_of(tile * BLK, BLK), BLK)
        high = (line // 256).astype(F32).astype(BF16)
        low = lax.rem(line, 256).astype(F32).astype(BF16)
        for kt in range(cc // 256):
            at = jnp.where(high == jnp.asarray(kt, BF16), low, jnp.full_like(low, -1.0))
            for j in range(16):
                hit = at == row16 + jnp.asarray(16.0 * j, BF16)
                dst[256 * kt + 16 * j : 256 * kt + 16 * j + 16, lanes] = jnp.where(
                    hit, jnp.ones((16, BLK), BF16), jnp.zeros((16, BLK), BF16)
                )

    c_fr.wait()
    c_fm.wait()
    kept = 2 * inst + 1 < HB_INST
    rows_of = lax.rem(lax.broadcasted_iota(jnp.int32, (BLK, BLK), 0), CB)
    block_of = lax.broadcasted_iota(jnp.int32, (16, BLK), 0) // 2 == lax.broadcasted_iota(jnp.int32, (16, BLK), 1) // CB
    drop = (lax.rem(lax.broadcasted_iota(jnp.int32, (2, BLK), 0), 2) == 0) | kept

    def restrict(tile):
        maps = [jnp.broadcast_to(fm_v[pl.ds(tile * 8 + e, 1), :], (CB, BLK)) for e in range(8)]
        onehot = jnp.where(rows_of == jnp.concatenate(maps, axis=0), 1.0, 0.0).astype(BF16)
        rows = pl.ds(pl.multiple_of(tile * 16, 16), 16)
        lanes = pl.ds(pl.multiple_of(tile * BLK, BLK), BLK)
        his, los = [], []
        for v in range(VARS):
            hi, lo = split2(fr_v[v, rows, :])
            his.append(hi)
            los.append(lo)
        got = dot_t(jnp.concatenate(his + los, axis=0), onehot)
        for v in range(VARS):
            both = jnp.where(block_of, got[16 * v : 16 * v + 16] + got[96 + 16 * v : 112 + 16 * v], 0.0)
            half = both[0:8] + both[8:16]
            half = half[0:4] + half[4:8]
            yu[v // 2, 2 * (v % 2) : 2 * (v % 2) + 2, lanes] = jnp.where(drop, half[0:2] + half[2:4], 0.0)

    def restrict_some(step, _):
        for u in range(4):
            restrict(step * 4 + u)
            permutation_tile(inv_v, perm, step * 4 + u)
        return 0

    lax.fori_loop(0, cc // BLK // 4, restrict_some, 0)
    terms = split3(jnp.concatenate([yu[0], yu[1], yu[2], yu[2]], axis=0))
    terms = jnp.concatenate(terms, axis=0)
    for nt in (0, cc // 256 - 1, *range(1, cc // 256 - 1)):
        got = dot(terms, perm[:, 256 * nt : 256 * nt + 256])
        got = got[0:16] + got[16:32] + got[32:48]
        for g in range(SWEEPERS):
            ysend[g, :, 256 * nt : 256 * nt + 256] = got[4 * g : 4 * g + 4, :]

    c_rl.wait()
    lsend[...] = jnp.zeros_like(lsend)
    lsend[:, : PEERS * HS] = rl_v[...]

    pl.semaphore_wait(barrier, partners)

    def taken_all(ref, sem):
        pltpu.make_async_copy(ref, ref, sem).wait()

    def list_copy(t):
        return pltpu.make_async_remote_copy(
            src_ref=lsend, dst_ref=lrx.at[t], send_sem=out_sem.at[0], recv_sem=list_sem.at[0],
            device_id={"cell": at_cell(OFFSETS[t]), "inst": inst}, device_id_type=MESH,
        )

    def rest_copy(g, kind):
        if kind == 0:
            src, dst = ysend.at[g], rx.at[inst]
        else:
            src = ysend.at[g, :, pl.ds((0, cc - BLK)[kind - 1], BLK)]
            dst = rxe.at[kind - 1, inst]
        return pltpu.make_async_remote_copy(
            src_ref=src, dst_ref=dst, send_sem=out_sem.at[1 + min(kind, 1)], recv_sem=rest_sem.at[min(kind, 1)],
            device_id={"cell": at_cell((0, 1, -1)[kind]), "inst": g}, device_id_type=MESH,
        )

    def halo_copy(k, t):
        return pltpu.make_async_remote_copy(
            src_ref=xsend.at[k, t // 4], dst_ref=halo.at[k, t], send_sem=out_sem.at[3], recv_sem=halo_sem.at[k],
            device_id={"cell": at_cell(-OFFSETS[t]), "inst": inst}, device_id_type=MESH,
        )

    def back_copy(g, kind):
        if kind == 0:
            src, dst = xf.at[g], gx.at[inst]
        else:
            src = xf.at[g, :, pl.ds((0, cc - BLK)[kind - 1], BLK)]
            dst = gxe.at[kind - 1, inst]
        return pltpu.make_async_remote_copy(
            src_ref=src, dst_ref=dst, send_sem=out_sem.at[4 + min(kind, 1)], recv_sem=back_sem.at[min(kind, 1)],
            device_id={"cell": at_cell((0, -1, 1)[kind]), "inst": g}, device_id_type=MESH,
        )

    sweeping = inst < SWEEPERS

    @pl.when(sweeping)
    def _():
        for t in range(PEERS):
            list_copy(t).start()

    for kind in (1, 2):
        for g in range(SWEEPERS):
            rest_copy(g, kind).start()
    for g in range(SWEEPERS):
        @pl.when(inst != g)
        def _():
            rest_copy(g, 0).start()

        @pl.when(inst == g)
        def _():
            rx[g] = ysend[g]

    c_nb.wait()
    c_fw.wait()
    c_sc.wait()
    c_de.wait()
    ids = [jnp.broadcast_to(nb_v[s : s + 1, :], (8, cc)) for s in range(NB)]
    face = [jnp.broadcast_to(fw_v[s : s + 1, :], (8, cc)) for s in range(NB)]
    total = face[0]
    for s in range(1, NB):
        total = total + face[s]
    for s in range(NB):
        for o in range(s + 1, NB):
            same = ids[s] == ids[o]
            face[s] = face[s] + jnp.where(same, face[o], 0.0)
            ids[o] = jnp.where(same, 2047, ids[o])

    def twice(x):
        return jnp.concatenate([x, x], axis=0)

    for s in range(NB):
        rows = pl.ds(16 * s, 16)
        table[pl.ds(T_Q + 16 * s, 16), :] = twice((ids[s] // 256).astype(F32)).astype(BF16)
        table[pl.ds(T_R + 16 * s, 16), :] = twice((ids[s] % 256).astype(F32)).astype(BF16)
        hi, lo = split2(twice(face[s]))
        table[pl.ds(T_H + 16 * s, 16), :] = hi
        table[pl.ds(T_L + 16 * s, 16), :] = lo
    sig = jnp.broadcast_to(sc_v[0:1, :], (8, cc))
    pair = [
        jnp.where(inst == 0, de_v[v : v + 1, :], jnp.where(inst == 1, de_v[2 + v : 3 + v, :], de_v[4 + v : 5 + v, :]))
        for v in range(2)
    ]
    odd = lax.rem(lax.broadcasted_iota(jnp.int32, (8, cc), 0), 4) >= 2
    diag = total + 3.0 * sig + jnp.where(odd, jnp.broadcast_to(pair[1], (8, cc)), jnp.broadcast_to(pair[0], (8, cc)))
    for k, part in enumerate(split3(twice(sig))):
        table[pl.ds(T_S + 16 * k, 16), :] = part
    for k, part in enumerate(split3(twice(diag))):
        table[pl.ds(T_D + 16 * k, 16), :] = part
    sg_v[:, SEND:] = twice(sig)
    di_v[:, SEND:] = twice(1.0 / diag)

    row = lax.broadcasted_iota(jnp.int32, (ROWS, BLK), 0)
    row_n = 2 * (row // 4) + row % 2
    row_v = (row % 4) // 2
    live = [p for p in range(ROWS) if 2 * (p // 4) + p % 2 < HB_INST]
    for slot, p in enumerate(live):
        n, v = 2 * (p // 4) + p % 2, (p % 4) // 2
        value = jnp.zeros((ROWS, BLK), F32)
        for m in range(HB_INST):
            value = jnp.where((row_n == m) & (row_v == v), spectral_value(m - n), value)
        coef[slot] = value

    quarter = lax.broadcasted_iota(jnp.int32, (ROWS, BLK), 1) // HS

    def build(src, lane_tiles, first_tile):
        def one(m, _):
            lt, kt = m // 5, lax.rem(m, 5)
            s_lanes = pl.ds(pl.multiple_of(lt * BLK, BLK), BLK)
            d_lanes = pl.ds(pl.multiple_of((lt + first_tile) * BLK, BLK), BLK)
            kf = kt.astype(F32).astype(BF16)
            at = []
            for s in range(NB):
                q = src[pl.ds(T_Q + 16 * s, 16), s_lanes]
                r = src[pl.ds(T_R + 16 * s, 16), s_lanes]
                at.append(jnp.where(q == kf, r, jnp.full_like(r, -1.0)))
            hs = [src[pl.ds(T_H + 16 * s, 16), s_lanes] for s in range(NB)]
            ls = [src[pl.ds(T_L + 16 * s, 16), s_lanes] for s in range(NB)]
            for j in range(16):
                here = row16 + jnp.asarray(16.0 * j, BF16)
                h = jnp.zeros((16, BLK), BF16)
                low = jnp.zeros((16, BLK), BF16)
                for s in range(NB):
                    hit = at[s] == here
                    h = jnp.where(hit, hs[s], h)
                    low = jnp.where(hit, ls[s], low)
                k_rows = pl.ds(pl.multiple_of(kt * 256 + 16 * j, 16), 16)
                wh[k_rows, d_lanes] = h
                wl[k_rows, d_lanes] = low
            return 0

        lax.fori_loop(*(5 * tile for tile in lane_tiles), one, 0)

    def local_part(x_all):
        own_hi, own_lo = split2(x_all[:, SEND:])
        xh_v[0:16, :] = own_hi
        xh_v[16:32, :] = own_lo
        x_v[...] = x_all
        for nt in range((SEND + cc) // 256):
            lanes = pl.ds(256 * nt, 256)
            a = dot(xh_v[...], wh[0:cc, lanes])
            b = dot(xh_v[0:16, :], wl[0:cc, lanes])
            halves = []
            for e in range(2):
                part = pl.ds(256 * nt + 128 * e, 128)
                acc = jnp.zeros((ROWS, BLK), F32)
                for slot, p in enumerate(live):
                    acc = acc + coef[slot] * jnp.broadcast_to(x_v[p : p + 1, part], (ROWS, BLK))
                halves.append(acc)
            sx = jnp.concatenate(halves, axis=1)
            base_v[:, lanes] = r_v[:, lanes] - sg_v[:, lanes] * sx + (a[0:16] + a[16:32] + b)

    def halo_rows(k):
        taken_all(halo.at[k], halo_sem.at[k])
        first = halo[k, 0]
        for t in range(1, 4):
            first = jnp.where(quarter == t, halo[k, t], first)
        second = jnp.where(quarter == 0, halo[k, 4], jnp.where(quarter == 1, halo[k, 5], 0.0))
        hi, lo = split2(jnp.concatenate([first, second], axis=1))
        return jnp.concatenate([hi, lo], axis=0)

    def with_halo(rows, lanes):
        a = dot(rows, wh[cc : cc + 256, lanes])
        b = dot(rows[0:16], wl[cc : cc + 256, lanes])
        return (base_v[:, lanes] + (a[0:16] + a[16:32] + b)) * di_v[:, lanes]

    def send_halo(k, x_send):
        xsend[k, 0] = x_send[:, 0:BLK]
        xsend[k, 1] = x_send[:, BLK:SEND]
        for t in range(PEERS):
            halo_copy(k, t).start()

    @pl.when(sweeping)
    def _():
        early = cc // BLK * 5 // 8
        build(table, (0, early), SEND // BLK)
        taken_all(lrx, list_sem.at[0])
        lane_slot = lax.broadcasted_iota(jnp.int32, (1, SEND), 1) // HS
        wanted = jnp.full((1, SEND), 4096, jnp.int32)
        for t in range(PEERS):
            wanted = jnp.where(lane_slot == t, lrx[t], wanted)
        for kt in range(cc // 256):
            rows256 = lax.broadcasted_iota(jnp.int32, (256, SEND), 0) + 256 * kt
            sel[256 * kt : 256 * kt + 256, :] = jnp.where(rows256 == wanted, 1.0, 0.0).astype(BF16)
        taken = dot(table[...], sel[...])
        stable[...] = taken[0:T_S].astype(BF16)
        used = lane_slot < PEERS
        sg_v[:, 0:SEND] = taken[T_S : T_S + 16] + taken[T_S + 16 : T_S + 32] + taken[T_S + 32 : T_S + 48]
        d_send = taken[T_D : T_D + 16] + taken[T_D + 16 : T_D + 32] + taken[T_D + 32 : T_D + 48]
        di_v[:, 0:SEND] = 1.0 / jnp.where(used, d_send, 1.0)
        taken_all(rxe, rest_sem.at[1])
        taken_all(rx.at[0 : n_inst - 1], rest_sem.at[0])
        lane = lax.broadcasted_iota(jnp.int32, (ROWS, BLK), 1)
        mine = jnp.concatenate([rx[src] for src in range(n_inst)], axis=0)
        low = jnp.concatenate([rxe[0, src] for src in range(n_inst)], axis=0)
        high = jnp.concatenate([rxe[1, src] for src in range(n_inst)], axis=0)
        edge = handed * CB
        rest = jnp.concatenate(
            [
                jnp.where(lane < edge, low, mine[:, 0:BLK]),
                mine[:, BLK : cc - BLK],
                jnp.where(lane >= BLK - edge, high, mine[:, cc - BLK :]),
            ],
            axis=1,
        )
        parts = dot(jnp.concatenate(split3(rest), axis=0), sel[...])
        r_send = parts[0:16] + parts[16:32] + parts[32:48]
        x_send = r_send * di_v[:, 0:SEND]
        send_halo(0, x_send)
        build(table, (early, cc // BLK), SEND // BLK)
        build(stable, (0, SEND // BLK), 0)
        r_v[:, 0:SEND] = r_send
        r_v[:, SEND:] = rest
        local_part(jnp.concatenate([x_send, rest * di_v[:, SEND:]], axis=1))

        def sweep(k, _):
            rows = halo_rows(k)
            x_send = with_halo(rows, pl.ds(0, SEND))
            send_halo(k + 1, x_send)
            parts = [x_send]
            for nt in range(cc // 256):
                parts.append(with_halo(rows, pl.ds(SEND + 256 * nt, 256)))
            local_part(jnp.concatenate(parts, axis=1))
            return 0

        lax.fori_loop(0, ITERS - 1, sweep, 0)
        rows = halo_rows(ITERS - 1)
        for nt in (0, cc // 256 - 1, *range(1, cc // 256 - 1)):
            out = with_halo(rows, pl.ds(SEND + 256 * nt, 256))
            for g in range(n_inst):
                xf[g, :, 256 * nt : 256 * nt + 256] = out[4 * g : 4 * g + 4, :]
            if nt == cc // 256 - 1:
                for kind in (1, 2):
                    for g in range(n_inst):
                        back_copy(g, kind).start()
        for g in range(n_inst):
            @pl.when(inst != g)
            def _():
                back_copy(g, 0).start()

            @pl.when(inst == g)
            def _():
                if g < SWEEPERS:
                    gx[g] = xf[g]

    def permute_back(step, _):
        for u in range(2):
            permutation_tile(pos_v, perm_t, step * 2 + u)
        return 0

    lax.fori_loop(0, cc // BLK // 2, permute_back, 0)
    taken_all(gxe, back_sem.at[1])

    @pl.when(sweeping)
    def _():
        taken_all(gx.at[0 : SWEEPERS - 1], back_sem.at[0])

    @pl.when(jnp.logical_not(sweeping))
    def _():
        taken_all(gx, back_sem.at[0])

    lane4 = lax.broadcasted_iota(jnp.int32, (4, BLK), 1)
    edge = handed * CB
    placed = []
    for src in range(SWEEPERS):
        own = gx[src]
        first = jnp.where(lane4 < edge, gxe[0, src], own[:, 0:BLK])
        last = jnp.where(lane4 >= BLK - edge, gxe[1, src], own[:, cc - BLK :])
        coarse_o[src] = own
        placed.append(jnp.concatenate([first, own[:, BLK : cc - BLK], last], axis=1))
    terms = jnp.concatenate(split3(jnp.concatenate(placed + placed[2:], axis=0)), axis=0)
    for nt in range(cc // 256):
        got = dot(terms, perm_t[:, 256 * nt : 256 * nt + 256])
        got = got[0:16] + got[16:32] + got[32:48]
        for g in range(SWEEPERS):
            blocks_o[g, :, 256 * nt : 256 * nt + 256] = got[4 * g : 4 * g + 4, :]

    taken_all(ysend.at[:, :, 0:256], out_sem.at[2])

    @pl.when(sweeping)
    def _():
        taken_all(ysend.at[0 : SWEEPERS - 1], out_sem.at[1])
        taken_all(lrx, out_sem.at[0])
        taken_all(halo, out_sem.at[3])
        taken_all(xf.at[0 : n_inst - 1], out_sem.at[4])
        taken_all(xf.at[:, :, 0:256], out_sem.at[5])

    @pl.when(jnp.logical_not(sweeping))
    def _():
        taken_all(ysend, out_sem.at[1])


def prolong(fm, coarse, blocks_x, fine_o, coarse_o):
    for v in range(VARS):
        coarse_o[v] = coarse[v // 2, 2 * (v % 2) : 2 * (v % 2) + 2, :]
    for tile in range(blocks_x.shape[2] // BLK):
        lanes = pl.ds(tile * BLK, BLK)
        for half in range(2):
            maps = [
                jnp.broadcast_to(fm[tile * 8 + 4 * half + e : tile * 8 + 4 * half + e + 1, :], (2, BLK)) + (4 * half + e) * CB
                for e in range(4)
            ]
            index = jnp.concatenate(maps, axis=0)
            rows = pl.ds(16 * tile + 8 * half, 8)
            for v in range(VARS):
                x = blocks_x[v // 2, 2 * (v % 2) : 2 * (v % 2) + 2, lanes]
                x = jnp.concatenate([x, x, x, x], axis=0)
                fine_o[v, rows, :] = jnp.take_along_axis(x, index, axis=1, mode="promise_in_bounds")


def body(n_cell, fine_residual, fine_map, routes, receive_lists, neighbours, face_weights, spectral_coef, diag_extra):
    inst_dev, var_count, fine_dev = fine_residual.shape
    blocks = fine_dev // BLK
    cc = blocks * CB
    lanes = SEND + cc
    vmem = pltpu.VMEM
    dma = pltpu.SemaphoreType.DMA
    any_spec = pl.BlockSpec(memory_space=pl.ANY)
    out_spec = pl.BlockSpec(memory_space=pltpu.VMEM)
    fine_rows = fine_residual.reshape(inst_dev, var_count, blocks, BLK).transpose(1, 2, 0, 3)
    fine_rows = fine_rows.reshape(var_count, blocks * inst_dev, BLK)
    cells_map = fine_map.reshape(blocks, BLK)
    coarse, in_blocks = pl.pallas_call(
        functools.partial(kernel, n_cell),
        out_shape=(
            jax.ShapeDtypeStruct((SWEEPERS, 4, cc), F32),
            jax.ShapeDtypeStruct((SWEEPERS, 4, cc), F32),
        ),
        in_specs=[any_spec] * 8,
        out_specs=(out_spec, out_spec),
        scratch_shapes=[
            vmem(fine_rows.shape, F32),
            vmem((blocks, BLK), jnp.int32),
            pltpu.SMEM((1, blocks), jnp.int32),
            vmem((1, PEERS * HS), jnp.int32),
            vmem((NB, cc), jnp.int32),
            vmem((NB, cc), F32),
            vmem((1, cc), F32),
            vmem((VARS, cc), F32),
            vmem((8, BLK), jnp.int32),
            vmem((8, BLK), jnp.int32),
            vmem((cc, cc), BF16),
            vmem((cc, cc), BF16),
            vmem((SWEEPERS, 4, cc), F32),
            vmem((SWEEPERS, 4, cc), F32),
            vmem((4, 4, cc), F32),
            vmem((2, 4, 4, BLK), F32),
            vmem((1, SEND), jnp.int32),
            vmem((PEERS, 1, SEND), jnp.int32),
            vmem((T_END, cc), BF16),
            vmem((T_S, SEND), BF16),
            vmem((cc, SEND), BF16),
            vmem((cc + 256, lanes), BF16),
            vmem((cc + 256, lanes), BF16),
            vmem((2 * HB_INST, ROWS, BLK), F32),
            vmem((ROWS, lanes), F32),
            vmem((ROWS, lanes), F32),
            vmem((ROWS, lanes), F32),
            vmem((ROWS, lanes), F32),
            vmem((ROWS, lanes), F32),
            vmem((2 * ROWS, cc), BF16),
            vmem((ITERS, 2, ROWS, BLK), F32),
            vmem((ITERS, PEERS, ROWS, BLK), F32),
            vmem((4, 4, cc), F32),
            vmem((SWEEPERS, 4, cc), F32),
            vmem((2, SWEEPERS, 4, BLK), F32),
            dma((8,)),
            dma((6,)),
            dma((1,)),
            dma((2,)),
            dma((ITERS,)),
            dma((2,)),
        ],
        compiler_params=pltpu.CompilerParams(collective_id=0, has_side_effects=True),
        name="multigrid",
    )(
        fine_rows,
        cells_map,
        routes,
        receive_lists,
        neighbours,
        face_weights,
        spectral_coef.reshape(1, cc),
        diag_extra,
    )
    fine, coarse = pl.pallas_call(
        prolong,
        out_shape=(
            jax.ShapeDtypeStruct(fine_rows.shape, F32),
            jax.ShapeDtypeStruct((var_count, inst_dev, cc), F32),
        ),
        in_specs=[out_spec] * 3,
        out_specs=(out_spec, out_spec),
        name="prolong",
    )(cells_map, coarse, in_blocks)
    fine = fine.reshape(var_count, blocks, inst_dev, BLK).transpose(2, 0, 1, 3).reshape(inst_dev, var_count, fine_dev)
    return fine, coarse.transpose(1, 0, 2)


def solution(mesh):
    in_specs = (
        P("inst", None, "cell"),
        P("cell"),
        P("cell", None),
        P("cell", None),
        P(None, "cell"),
        P(None, "cell"),
        P("cell"),
        P(None, "cell"),
    )
    out_specs = (P("inst", None, "cell"), P("inst", None, "cell"))
    return jax.shard_map(
        functools.partial(body, mesh.shape["cell"]), mesh=mesh, in_specs=in_specs, out_specs=out_specs, check_vma=False
    )
```

```python
import functools
import math

import jax
import jax.numpy as jnp
from jax import lax
from jax.experimental import pallas as pl
from jax.experimental.pallas import tpu as pltpu
from jax.sharding import PartitionSpec as P

INST = 8
HB_INST = 7
VARS = 6
NB = 6
BLK = 128
CB = 16
RAD = 3
HS = 32
ITERS = 6
PEERS = 2 * RAD
OFFSETS = [t - RAD if t < RAD else t - RAD + 1 for t in range(PEERS)]
SWEEPERS = 3
ROWS = 16
SEND = 256
MESH = pl.DeviceIdType.MESH
F32 = jnp.float32
BF16 = jnp.bfloat16
T_Q, T_R, T_H, T_L, T_END = 0, 6, 12, 18, 24
PLANE, CORES = 8, 2


def spectral_value(distance):
    if distance == 0:
        return 0.0
    sign = -1.0 if distance % 2 else 1.0
    return 0.5 * sign / math.sin(math.pi * distance / HB_INST)


def split2(x):
    hi = x.astype(BF16)
    return hi, (x - hi.astype(F32)).astype(BF16)


def split3(x):
    hi = x.astype(BF16)
    rest = x - hi.astype(F32)
    mid = rest.astype(BF16)
    return hi, mid, (rest - mid.astype(F32)).astype(BF16)


def dot(a, b):
    return lax.dot_general(a, b, (((1,), (0,)), ((), ())), preferred_element_type=F32)


def dot_t(a, b):
    return lax.dot_general(a, b, (((1,), (1,)), ((), ())), preferred_element_type=F32)


def kernel(
    n_cell,
    fr, fm, rt, rl, nb, fw, sc, de,
    coarse_o, blocks_o,
    fr_v, fm_v, rt_s, rl_v, nb_v, fw_v, sc_v, de_v,
    inv_v, pos_v, perm, perm_t, yu,
    ysend, rx, rxe, lsend, lrx, dsend, drx, nb_r, fw_r,
    table, stable, sel, wh, wl, coef,
    r_v, sg_v, di_v, base_v, x_v, xh_v,
    xsend, halo, xf, gx, gxe,
    in_sem, out_sem, list_sem, move_sem, rest_sem, halo_sem, back_sem,
):
    cell = lax.axis_index("cell")
    inst = lax.axis_index("inst")
    blocks = fm_v.shape[0]
    handed = blocks // 16
    cc = blocks * CB
    n_inst = 4

    def wrap(c):
        return lax.rem(c + n_cell, n_cell)

    def mirror(c):
        z, place = lax.div(c, PLANE), lax.rem(c, PLANE)
        core = lax.rem(place, CORES)
        return jnp.where(lax.rem(z, 2) == 1, z * PLANE + (PLANE - CORES) - (place - core) + core, c)

    me = mirror(cell)
    swapped = me != cell

    def copy_in(i, src, dst):
        c = pltpu.make_async_copy(src, dst, in_sem.at[i])
        c.start()
        return c

    c_rt = copy_in(0, rt, rt_s)
    c_fr = copy_in(1, fr, fr_v)
    c_fm = copy_in(2, fm, fm_v)
    c_rl = copy_in(3, rl, rl_v)
    c_nb = copy_in(4, nb, nb_v)
    c_fw = copy_in(5, fw, fw_v)
    c_sc = copy_in(6, sc, sc_v)
    c_de = copy_in(7, de, de_v)

    barrier = pltpu.get_barrier_semaphore()

    def greet(c, i):
        pl.semaphore_signal(barrier, inc=1, device_id={"cell": c, "inst": i}, device_id_type=MESH)

    def others(c):
        for j in range(n_inst):
            greet(c, lax.rem(inst + j, n_inst))

    partners = jnp.int32(3)
    for j in range(1, n_inst):
        greet(me, lax.rem(inst + j, n_inst))

    @pl.when(swapped)
    def _():
        greet(me, inst)

    partners = partners + jnp.where(swapped, 1, 0)
    for d in (-1, 1):
        others(mirror(wrap(cell + d)))
        others(wrap(me + d))
        partners = partners + 2 * n_inst
    for d in (-3, -2, 2, 3):
        for target in (mirror(wrap(cell + d)), wrap(me - d)):
            @pl.when(target != cell)
            def _():
                greet(target, inst)

            partners = partners + jnp.where(target != cell, 1, 0)
    for d in OFFSETS:
        greet(mirror(wrap(me + d)), inst)
        partners = partners + 1

    c_rt.wait()
    group = lax.broadcasted_iota(jnp.int32, (8, BLK), 0) * 8 + lax.broadcasted_iota(jnp.int32, (8, BLK), 1) // CB

    above = wrap(cell + 1)

    def find(step, carry):
        c0, c1, inv, fwd = carry
        for u in range(8):
            b = step * 8 + u
            route = rt_s[0, b]
            is0 = route == above
            is1 = route == cell
            pos = jnp.where(is1, c1, jnp.where(is0, c0, blocks + b - c0 - c1))
            c0 = c0 + jnp.where(is0, 1, 0)
            c1 = c1 + jnp.where(is1, 1, 0)
            inv = jnp.where(group == pos, b, inv)
            fwd = jnp.where(group == b, pos, fwd)
        return c0, c1, inv, fwd

    zero8 = jnp.zeros((8, BLK), jnp.int32)
    found = lax.fori_loop(0, blocks // 8, find, (jnp.int32(0), jnp.int32(handed), zero8, zero8))
    within = lax.rem(lax.broadcasted_iota(jnp.int32, (8, BLK), 1), CB)
    inv_v[...] = found[2] * CB + within
    pos_v[...] = found[3] * CB + within

    row16 = lax.broadcasted_iota(jnp.int32, (16, BLK), 0).astype(F32).astype(BF16)

    def permutation_tile(src, dst, tile):
        line = jnp.broadcast_to(src[pl.ds(tile, 1), :], (16, BLK))
        lanes = pl.ds(pl.multiple_of(tile * BLK, BLK), BLK)
        high = (line // 256).astype(F32).astype(BF16)
        low = lax.rem(line, 256).astype(F32).astype(BF16)
        for kt in range(cc // 256):
            at = jnp.where(high == jnp.asarray(kt, BF16), low, jnp.full_like(low, -1.0))
            for j in range(16):
                hit = at == row16 + jnp.asarray(16.0 * j, BF16)
                dst[256 * kt + 16 * j : 256 * kt + 16 * j + 16, lanes] = jnp.where(
                    hit, jnp.ones((16, BLK), BF16), jnp.zeros((16, BLK), BF16)
                )

    c_fr.wait()
    c_fm.wait()
    kept = 2 * inst + 1 < HB_INST
    rows_of = lax.rem(lax.broadcasted_iota(jnp.int32, (BLK, BLK), 0), CB)
    block_of = lax.broadcasted_iota(jnp.int32, (16, BLK), 0) // 2 == lax.broadcasted_iota(jnp.int32, (16, BLK), 1) // CB
    drop = (lax.rem(lax.broadcasted_iota(jnp.int32, (2, BLK), 0), 2) == 0) | kept

    def restrict(tile):
        maps = [jnp.broadcast_to(fm_v[pl.ds(tile * 8 + e, 1), :], (CB, BLK)) for e in range(8)]
        onehot = jnp.where(rows_of == jnp.concatenate(maps, axis=0), 1.0, 0.0).astype(BF16)
        rows = pl.ds(pl.multiple_of(tile * 16, 16), 16)
        lanes = pl.ds(pl.multiple_of(tile * BLK, BLK), BLK)
        his, los = [], []
        for v in range(VARS):
            hi, lo = split2(fr_v[v, rows, :])
            his.append(hi)
            los.append(lo)
        got = dot_t(jnp.concatenate(his + los, axis=0), onehot)
        for v in range(VARS):
            both = jnp.where(block_of, got[16 * v : 16 * v + 16] + got[96 + 16 * v : 112 + 16 * v], 0.0)
            half = both[0:8] + both[8:16]
            half = half[0:4] + half[4:8]
            yu[v // 2, 2 * (v % 2) : 2 * (v % 2) + 2, lanes] = jnp.where(drop, half[0:2] + half[2:4], 0.0)

    def restrict_some(step, _):
        for u in range(4):
            restrict(step * 4 + u)
            permutation_tile(inv_v, perm, step * 4 + u)
        return 0

    lax.fori_loop(0, cc // BLK // 4, restrict_some, 0)
    terms = split3(jnp.concatenate([yu[0], yu[1], yu[2], yu[2]], axis=0))
    terms = jnp.concatenate(terms, axis=0)
    for nt in (0, cc // 256 - 1, *range(1, cc // 256 - 1)):
        got = dot(terms, perm[:, 256 * nt : 256 * nt + 256])
        got = got[0:16] + got[16:32] + got[32:48]
        for g in range(SWEEPERS):
            ysend[g, :, 256 * nt : 256 * nt + 256] = got[4 * g : 4 * g + 4, :]

    c_rl.wait()
    lsend[...] = jnp.zeros_like(lsend)
    lsend[:, : PEERS * HS] = rl_v[...]

    c_nb.wait()
    c_fw.wait()
    c_sc.wait()
    c_de.wait()
    total = fw_v[0:1, :]
    for s in range(1, NB):
        total = total + fw_v[s : s + 1, :]
    total = total + 3.0 * sc_v[...]
    for v in range(2):
        extra = jnp.where(
            inst == 0, de_v[v : v + 1, :], jnp.where(inst == 1, de_v[2 + v : 3 + v, :], de_v[4 + v : 5 + v, :])
        )
        dsend[v : v + 1, :] = total + extra
    dsend[2:3, :] = sc_v[...]
    dsend[3:4, :] = sc_v[...]

    pl.semaphore_wait(barrier, partners)

    def taken_all(ref, sem):
        pltpu.make_async_copy(ref, ref, sem).wait()

    def list_copy(t):
        return pltpu.make_async_remote_copy(
            src_ref=lsend, dst_ref=lrx.at[t], send_sem=out_sem.at[0], recv_sem=list_sem.at[0],
            device_id={"cell": mirror(wrap(cell + OFFSETS[t])), "inst": inst}, device_id_type=MESH,
        )

    moves = ((dsend, drx), (nb_v, nb_r), (fw_v, fw_r))

    def move_copy(m):
        return pltpu.make_async_remote_copy(
            src_ref=moves[m][0], dst_ref=moves[m][1], send_sem=out_sem.at[6 + m], recv_sem=move_sem.at[m],
            device_id={"cell": me, "inst": inst}, device_id_type=MESH,
        )

    def move(m):
        @pl.when(swapped)
        def _():
            move_copy(m).start()

        @pl.when(jnp.logical_not(swapped))
        def _():
            pltpu.make_async_copy(*moves[m], move_sem.at[m]).start()

    def rest_copy(g, kind):
        if kind == 0:
            src, dst = ysend.at[g], rx.at[inst]
        else:
            src = ysend.at[g, :, pl.ds((0, cc - BLK)[kind - 1], BLK)]
            dst = rxe.at[kind - 1, inst]
        return pltpu.make_async_remote_copy(
            src_ref=src, dst_ref=dst, send_sem=out_sem.at[1 + min(kind, 1)], recv_sem=rest_sem.at[min(kind, 1)],
            device_id={"cell": mirror(wrap(cell + (0, 1, -1)[kind])), "inst": g}, device_id_type=MESH,
        )

    def halo_copy(k, t):
        return pltpu.make_async_remote_copy(
            src_ref=xsend.at[k, t // 4], dst_ref=halo.at[k, t], send_sem=out_sem.at[3], recv_sem=halo_sem.at[k],
            device_id={"cell": mirror(wrap(me - OFFSETS[t])), "inst": inst}, device_id_type=MESH,
        )

    def back_copy(g, kind):
        if kind == 0:
            src, dst = xf.at[g], gx.at[inst]
        else:
            src = xf.at[g, :, pl.ds((0, cc - BLK)[kind - 1], BLK)]
            dst = gxe.at[kind - 1, inst]
        return pltpu.make_async_remote_copy(
            src_ref=src, dst_ref=dst, send_sem=out_sem.at[4 + min(kind, 1)], recv_sem=back_sem.at[min(kind, 1)],
            device_id={"cell": wrap(me + (0, -1, 1)[kind]), "inst": g}, device_id_type=MESH,
        )

    sweeping = inst < SWEEPERS

    @pl.when(sweeping)
    def _():
        for t in range(PEERS):
            if abs(OFFSETS[t]) == 2:
                here = mirror(wrap(cell + OFFSETS[t])) == cell

                @pl.when(here)
                def _():
                    pltpu.make_async_copy(lsend, lrx.at[t], list_sem.at[0]).start()

                @pl.when(jnp.logical_not(here))
                def _():
                    list_copy(t).start()
            else:
                list_copy(t).start()

    for kind in (1, 2):
        for g in range(SWEEPERS):
            rest_copy(g, kind).start()

    @pl.when(sweeping)
    def _():
        move(0)

    for g in range(SWEEPERS):
        local = (inst == g) & jnp.logical_not(swapped)

        @pl.when(jnp.logical_not(local))
        def _():
            rest_copy(g, 0).start()

        @pl.when(local)
        def _():
            pltpu.make_async_copy(ysend.at[g], rx.at[g], rest_sem.at[0]).start()

    @pl.when(sweeping)
    def _():
        move(1)
        move(2)

    row = lax.broadcasted_iota(jnp.int32, (ROWS, BLK), 0)
    row_n = 2 * (row // 4) + row % 2
    row_v = (row % 4) // 2
    live = [p for p in range(ROWS) if 2 * (p // 4) + p % 2 < HB_INST]
    for slot, p in enumerate(live):
        n, v = 2 * (p // 4) + p % 2, (p % 4) // 2
        value = jnp.zeros((ROWS, BLK), F32)
        for m in range(HB_INST):
            value = jnp.where((row_n == m) & (row_v == v), spectral_value(m - n), value)
        coef[slot] = value

    quarter = lax.broadcasted_iota(jnp.int32, (ROWS, BLK), 1) // HS

    def build(src, lane_tiles, first_tile):
        def one(m, _):
            lt, kt = m // 5, lax.rem(m, 5)
            s_lanes = pl.ds(pl.multiple_of(lt * BLK, BLK), BLK)
            d_lanes = pl.ds(pl.multiple_of((lt + first_tile) * BLK, BLK), BLK)
            kf = kt.astype(F32).astype(BF16)
            at = []
            def line(i):
                return jnp.broadcast_to(src[i : i + 1, s_lanes], (16, BLK)).astype(BF16)

            for s in range(NB):
                r = line(T_R + s)
                at.append(jnp.where(line(T_Q + s) == kf, r, jnp.full_like(r, -1.0)))
            hs = [line(T_H + s) for s in range(NB)]
            ls = [line(T_L + s) for s in range(NB)]
            for j in range(16):
                here = row16 + jnp.asarray(16.0 * j, BF16)
                h = jnp.zeros((16, BLK), BF16)
                low = jnp.zeros((16, BLK), BF16)
                for s in range(NB):
                    hit = at[s] == here
                    h = jnp.where(hit, hs[s], h)
                    low = jnp.where(hit, ls[s], low)
                k_rows = pl.ds(pl.multiple_of(kt * 256 + 16 * j, 16), 16)
                wh[k_rows, d_lanes] = h
                wl[k_rows, d_lanes] = low
            return 0

        lax.fori_loop(*(5 * tile for tile in lane_tiles), one, 0)

    def local_part(x_all):
        own_hi, own_lo = split2(x_all[:, SEND:])
        xh_v[0:16, :] = own_hi
        xh_v[16:32, :] = own_lo
        x_v[...] = x_all
        for nt in range((SEND + cc) // 256):
            lanes = pl.ds(256 * nt, 256)
            a = dot(xh_v[...], wh[0:cc, lanes])
            b = dot(xh_v[0:16, :], wl[0:cc, lanes])
            halves = []
            for e in range(2):
                part = pl.ds(256 * nt + 128 * e, 128)
                acc = jnp.zeros((ROWS, BLK), F32)
                for slot, p in enumerate(live):
                    acc = acc + coef[slot] * jnp.broadcast_to(x_v[p : p + 1, part], (ROWS, BLK))
                halves.append(acc)
            sx = jnp.concatenate(halves, axis=1)
            base_v[:, lanes] = r_v[:, lanes] - sg_v[:, lanes] * sx + (a[0:16] + a[16:32] + b)

    def halo_rows(k):
        taken_all(halo.at[k], halo_sem.at[k])
        first = halo[k, 0]
        for t in range(1, 4):
            first = jnp.where(quarter == t, halo[k, t], first)
        second = jnp.where(quarter == 0, halo[k, 4], jnp.where(quarter == 1, halo[k, 5], 0.0))
        hi, lo = split2(jnp.concatenate([first, second], axis=1))
        return jnp.concatenate([hi, lo], axis=0)

    def with_halo(rows, lanes):
        a = dot(rows, wh[cc : cc + 256, lanes])
        b = dot(rows[0:16], wl[cc : cc + 256, lanes])
        return (base_v[:, lanes] + (a[0:16] + a[16:32] + b)) * di_v[:, lanes]

    def send_halo(k, x_send):
        xsend[k, 0] = x_send[:, 0:BLK]
        xsend[k, 1] = x_send[:, BLK:SEND]
        for t in range(PEERS):
            halo_copy(k, t).start()

    @pl.when(sweeping)
    def _():
        def own_matrix():
            taken_all(nb_r, move_sem.at[1])
            taken_all(fw_r, move_sem.at[2])
            ids = [jnp.broadcast_to(nb_r[s : s + 1, :], (8, cc)) for s in range(NB)]
            face = [jnp.broadcast_to(fw_r[s : s + 1, :], (8, cc)) for s in range(NB)]
            for s in range(NB):
                for o in range(s + 1, NB):
                    same = ids[s] == ids[o]
                    face[s] = face[s] + jnp.where(same, face[o], 0.0)
                    ids[o] = jnp.where(same, 2047, ids[o])
            for s in range(NB):
                table[T_Q + s : T_Q + s + 1, :] = lax.shift_right_logical(ids[s], 8).astype(F32)[0:1]
                table[T_R + s : T_R + s + 1, :] = (ids[s] & 255).astype(F32)[0:1]
                hi = face[s].astype(BF16).astype(F32)
                table[T_H + s : T_H + s + 1, :] = hi[0:1]
                table[T_L + s : T_L + s + 1, :] = (face[s] - hi).astype(BF16).astype(F32)[0:1]
            build(table, (0, cc // BLK), SEND // BLK)

        @pl.when(jnp.logical_not(swapped))
        def _():
            own_matrix()

        taken_all(lrx, list_sem.at[0])
        lane_slot = lax.broadcasted_iota(jnp.int32, (1, SEND), 1) // HS
        wanted = jnp.full((1, SEND), 4096, jnp.int32)
        for t in range(PEERS):
            wanted = jnp.where(lane_slot == t, lrx[t], wanted)
        for kt in range(cc // 256):
            rows256 = lax.broadcasted_iota(jnp.int32, (256, SEND), 0) + 256 * kt
            sel[256 * kt : 256 * kt + 256, :] = jnp.where(rows256 == wanted, 1.0, 0.0).astype(BF16)
        taken_all(drx, move_sem.at[0])
        late = dot(jnp.concatenate(split3(jnp.concatenate([drx[...], drx[...]], axis=0)), axis=0), sel[...])
        late = late[0:8] + late[8:16] + late[16:24]

        def by_variable(x, width):
            second = lax.rem(lax.broadcasted_iota(jnp.int32, (ROWS, width), 0), 4) >= 2
            return jnp.where(second, jnp.broadcast_to(x[1:2], (ROWS, width)), jnp.broadcast_to(x[0:1], (ROWS, width)))

        used = lane_slot < PEERS
        sg_v[:, 0:SEND] = jnp.broadcast_to(late[2:3], (ROWS, SEND))
        di_v[:, 0:SEND] = 1.0 / jnp.where(used, by_variable(late, SEND), 1.0)
        sg_v[:, SEND:] = jnp.broadcast_to(drx[2:3, :], (ROWS, cc))
        di_v[:, SEND:] = 1.0 / by_variable(drx[...], cc)
        taken_all(rxe, rest_sem.at[1])
        taken_all(rx, rest_sem.at[0])
        lane = lax.broadcasted_iota(jnp.int32, (ROWS, BLK), 1)
        mine = jnp.concatenate([rx[src] for src in range(n_inst)], axis=0)
        low = jnp.concatenate([rxe[0, src] for src in range(n_inst)], axis=0)
        high = jnp.concatenate([rxe[1, src] for src in range(n_inst)], axis=0)
        edge = handed * CB
        rest = jnp.concatenate(
            [
                jnp.where(lane < edge, low, mine[:, 0:BLK]),
                mine[:, BLK : cc - BLK],
                jnp.where(lane >= BLK - edge, high, mine[:, cc - BLK :]),
            ],
            axis=1,
        )
        parts = dot(jnp.concatenate(split3(rest), axis=0), sel[...])
        r_send = parts[0:16] + parts[16:32] + parts[32:48]
        x_send = r_send * di_v[:, 0:SEND]
        send_halo(0, x_send)

        @pl.when(swapped)
        def _():
            own_matrix()

        stable[...] = dot(table[...].astype(BF16), sel[...])
        build(stable, (0, SEND // BLK), 0)
        r_v[:, 0:SEND] = r_send
        r_v[:, SEND:] = rest
        local_part(jnp.concatenate([x_send, rest * di_v[:, SEND:]], axis=1))

        def sweep(k, _):
            rows = halo_rows(k)
            x_send = with_halo(rows, pl.ds(0, SEND))
            send_halo(k + 1, x_send)
            parts = [x_send]
            for nt in range(cc // 256):
                parts.append(with_halo(rows, pl.ds(SEND + 256 * nt, 256)))
            local_part(jnp.concatenate(parts, axis=1))
            return 0

        lax.fori_loop(0, ITERS - 1, sweep, 0)
        rows = halo_rows(ITERS - 1)
        for nt in (0, cc // 256 - 1, *range(1, cc // 256 - 1)):
            out = with_halo(rows, pl.ds(SEND + 256 * nt, 256))
            for g in range(n_inst):
                xf[g, :, 256 * nt : 256 * nt + 256] = out[4 * g : 4 * g + 4, :]
            if nt == cc // 256 - 1:
                for kind in (1, 2):
                    for g in range(n_inst):
                        back_copy(g, kind).start()
        for g in range(n_inst):
            local = (inst == g) & jnp.logical_not(swapped)

            @pl.when(jnp.logical_not(local))
            def _():
                back_copy(g, 0).start()

            if g < SWEEPERS:
                @pl.when(local)
                def _():
                    pltpu.make_async_copy(xf.at[g], gx.at[g], back_sem.at[0]).start()

    def permute_back(step, _):
        for u in range(2):
            permutation_tile(pos_v, perm_t, step * 2 + u)
        return 0

    lax.fori_loop(0, cc // BLK // 2, permute_back, 0)
    taken_all(gxe, back_sem.at[1])
    taken_all(gx, back_sem.at[0])
    lane4 = lax.broadcasted_iota(jnp.int32, (4, BLK), 1)
    edge = handed * CB
    placed = []
    for src in range(SWEEPERS):
        own = gx[src]
        first = jnp.where(lane4 < edge, gxe[0, src], own[:, 0:BLK])
        last = jnp.where(lane4 >= BLK - edge, gxe[1, src], own[:, cc - BLK :])
        coarse_o[src] = own
        placed.append(jnp.concatenate([first, own[:, BLK : cc - BLK], last], axis=1))
    terms = jnp.concatenate(split3(jnp.concatenate(placed + placed[2:], axis=0)), axis=0)
    for nt in range(cc // 256):
        got = dot(terms, perm_t[:, 256 * nt : 256 * nt + 256])
        got = got[0:16] + got[16:32] + got[32:48]
        for g in range(SWEEPERS):
            blocks_o[g, :, 256 * nt : 256 * nt + 256] = got[4 * g : 4 * g + 4, :]

    taken_all(ysend.at[:, :, 0:256], out_sem.at[2])

    @pl.when(sweeping & jnp.logical_not(swapped))
    def _():
        taken_all(ysend.at[0 : SWEEPERS - 1], out_sem.at[1])
        taken_all(xf.at[0 : n_inst - 1], out_sem.at[4])

    @pl.when(jnp.logical_not(sweeping) | swapped)
    def _():
        taken_all(ysend, out_sem.at[1])

    @pl.when(sweeping & swapped)
    def _():
        taken_all(xf, out_sem.at[4])
        for m in range(3):
            taken_all(moves[m][1], out_sem.at[6 + m])

    @pl.when(sweeping)
    def _():
        at_home = (mirror(wrap(cell + 2)) == cell) | (mirror(wrap(cell - 2)) == cell)

        @pl.when(at_home)
        def _():
            taken_all(lrx.at[0 : PEERS - 1], out_sem.at[0])

        @pl.when(jnp.logical_not(at_home))
        def _():
            taken_all(lrx, out_sem.at[0])

        taken_all(halo, out_sem.at[3])
        taken_all(xf.at[:, :, 0:256], out_sem.at[5])


def prolong(fm, coarse, blocks_x, fine_o, coarse_o):
    for v in range(VARS):
        coarse_o[v] = coarse[v // 2, 2 * (v % 2) : 2 * (v % 2) + 2, :]
    for tile in range(blocks_x.shape[2] // BLK):
        lanes = pl.ds(tile * BLK, BLK)
        for half in range(2):
            maps = [
                jnp.broadcast_to(fm[tile * 8 + 4 * half + e : tile * 8 + 4 * half + e + 1, :], (2, BLK)) + (4 * half + e) * CB
                for e in range(4)
            ]
            index = jnp.concatenate(maps, axis=0)
            rows = pl.ds(16 * tile + 8 * half, 8)
            for v in range(VARS):
                x = blocks_x[v // 2, 2 * (v % 2) : 2 * (v % 2) + 2, lanes]
                x = jnp.concatenate([x, x, x, x], axis=0)
                fine_o[v, rows, :] = jnp.take_along_axis(x, index, axis=1, mode="promise_in_bounds")


def body(n_cell, fine_residual, fine_map, routes, receive_lists, neighbours, face_weights, spectral_coef, diag_extra):
    inst_dev, var_count, fine_dev = fine_residual.shape
    blocks = fine_dev // BLK
    cc = blocks * CB
    lanes = SEND + cc
    vmem = pltpu.VMEM
    dma = pltpu.SemaphoreType.DMA
    any_spec = pl.BlockSpec(memory_space=pl.ANY)
    out_spec = pl.BlockSpec(memory_space=pltpu.VMEM)
    fine_rows = fine_residual.reshape(inst_dev, var_count, blocks, BLK).transpose(1, 2, 0, 3)
    fine_rows = fine_rows.reshape(var_count, blocks * inst_dev, BLK)
    cells_map = fine_map.reshape(blocks, BLK)
    coarse, in_blocks = pl.pallas_call(
        functools.partial(kernel, n_cell),
        out_shape=(
            jax.ShapeDtypeStruct((SWEEPERS, 4, cc), F32),
            jax.ShapeDtypeStruct((SWEEPERS, 4, cc), F32),
        ),
        in_specs=[any_spec] * 8,
        out_specs=(out_spec, out_spec),
        scratch_shapes=[
            vmem(fine_rows.shape, F32),
            vmem((blocks, BLK), jnp.int32),
            pltpu.SMEM((1, blocks), jnp.int32),
            vmem((1, PEERS * HS), jnp.int32),
            vmem((NB, cc), jnp.int32),
            vmem((NB, cc), F32),
            vmem((1, cc), F32),
            vmem((VARS, cc), F32),
            vmem((8, BLK), jnp.int32),
            vmem((8, BLK), jnp.int32),
            vmem((cc, cc), BF16),
            vmem((cc, cc), BF16),
            vmem((SWEEPERS, 4, cc), F32),
            vmem((SWEEPERS, 4, cc), F32),
            vmem((4, 4, cc), F32),
            vmem((2, 4, 4, BLK), F32),
            vmem((1, SEND), jnp.int32),
            vmem((PEERS, 1, SEND), jnp.int32),
            vmem((4, cc), F32),
            vmem((4, cc), F32),
            vmem((NB, cc), jnp.int32),
            vmem((NB, cc), F32),
            vmem((T_END, cc), F32),
            vmem((T_END, SEND), F32),
            vmem((cc, SEND), BF16),
            vmem((cc + 256, lanes), BF16),
            vmem((cc + 256, lanes), BF16),
            vmem((2 * HB_INST, ROWS, BLK), F32),
            vmem((ROWS, lanes), F32),
            vmem((ROWS, lanes), F32),
            vmem((ROWS, lanes), F32),
            vmem((ROWS, lanes), F32),
            vmem((ROWS, lanes), F32),
            vmem((2 * ROWS, cc), BF16),
            vmem((ITERS, 2, ROWS, BLK), F32),
            vmem((ITERS, PEERS, ROWS, BLK), F32),
            vmem((4, 4, cc), F32),
            vmem((SWEEPERS, 4, cc), F32),
            vmem((2, SWEEPERS, 4, BLK), F32),
            dma((8,)),
            dma((9,)),
            dma((1,)),
            dma((3,)),
            dma((2,)),
            dma((ITERS,)),
            dma((2,)),
        ],
        compiler_params=pltpu.CompilerParams(collective_id=0, has_side_effects=True),
        name="multigrid",
    )(
        fine_rows,
        cells_map,
        routes,
        receive_lists,
        neighbours,
        face_weights,
        spectral_coef.reshape(1, cc),
        diag_extra,
    )
    fine, coarse = pl.pallas_call(
        prolong,
        out_shape=(
            jax.ShapeDtypeStruct(fine_rows.shape, F32),
            jax.ShapeDtypeStruct((var_count, inst_dev, cc), F32),
        ),
        in_specs=[out_spec] * 3,
        out_specs=(out_spec, out_spec),
        name="prolong",
    )(cells_map, coarse, in_blocks)
    fine = fine.reshape(var_count, blocks, inst_dev, BLK).transpose(2, 0, 1, 3).reshape(inst_dev, var_count, fine_dev)
    return fine, coarse.transpose(1, 0, 2)


def solution(mesh):
    in_specs = (
        P("inst", None, "cell"),
        P("cell"),
        P("cell", None),
        P("cell", None),
        P(None, "cell"),
        P(None, "cell"),
        P("cell"),
        P(None, "cell"),
    )
    out_specs = (P("inst", None, "cell"), P("inst", None, "cell"))
    return jax.shard_map(
        functools.partial(body, mesh.shape["cell"]), mesh=mesh, in_specs=in_specs, out_specs=out_specs, check_vma=False
    )
```

```python
import functools
import math

import jax
import jax.numpy as jnp
from jax import lax
from jax.experimental import pallas as pl
from jax.experimental.pallas import tpu as pltpu
from jax.sharding import PartitionSpec as P

INST = 8
HB_INST = 7
VARS = 6
NB = 6
BLK = 128
CB = 16
RAD = 3
HS = 32
ITERS = 6
PEERS = 2 * RAD
OFFSETS = [t - RAD if t < RAD else t - RAD + 1 for t in range(PEERS)]
SWEEPERS = 3
ROWS = 16
SEND = 256
MESH = pl.DeviceIdType.MESH
F32 = jnp.float32
BF16 = jnp.bfloat16
T_Q, T_R, T_H, T_L, T_END = 0, 6, 12, 18, 24
PLANE, CORES = 8, 2
EARLY = 5


def spectral_value(distance):
    if distance == 0:
        return 0.0
    sign = -1.0 if distance % 2 else 1.0
    return 0.5 * sign / math.sin(math.pi * distance / HB_INST)


def split2(x):
    hi = x.astype(BF16)
    return hi, (x - hi.astype(F32)).astype(BF16)


def split3(x):
    hi = x.astype(BF16)
    rest = x - hi.astype(F32)
    mid = rest.astype(BF16)
    return hi, mid, (rest - mid.astype(F32)).astype(BF16)


def dot(a, b):
    return lax.dot_general(a, b, (((1,), (0,)), ((), ())), preferred_element_type=F32)


def dot_t(a, b):
    return lax.dot_general(a, b, (((1,), (1,)), ((), ())), preferred_element_type=F32)


def kernel(
    n_cell,
    fr, fm, rt, rl, nb, fw, sc, de,
    coarse_o, blocks_o,
    fr_v, fm_v, rt_s, rl_v, nb_v, fw_v, sc_v, de_v,
    inv_v, pos_v, perm, perm_t, yu,
    ysend, rx, rxe, lsend, lrx, dsend, drx, nb_r, fw_r,
    table, stable, sel, wh, wl, coef,
    r_v, sg_v, di_v, base_v, x_v, xh_v,
    xsend, halo, xf, gx, gxe,
    in_sem, out_sem, list_sem, move_sem, rest_sem, halo_sem, back_sem,
):
    cell = lax.axis_index("cell")
    inst = lax.axis_index("inst")
    blocks = fm_v.shape[0]
    handed = blocks // 16
    cc = blocks * CB
    n_inst = 4

    def wrap(c):
        return lax.rem(c + n_cell, n_cell)

    def mirror(c):
        z, place = lax.div(c, PLANE), lax.rem(c, PLANE)
        core = lax.rem(place, CORES)
        return jnp.where(lax.rem(z, 2) == 1, z * PLANE + (PLANE - CORES) - (place - core) + core, c)

    me = mirror(cell)
    swapped = me != cell

    def copy_in(i, src, dst):
        c = pltpu.make_async_copy(src, dst, in_sem.at[i])
        c.start()
        return c

    c_rt = copy_in(0, rt, rt_s)
    c_fr = copy_in(1, fr, fr_v)
    c_fm = copy_in(2, fm, fm_v)
    c_rl = copy_in(3, rl, rl_v)
    c_nb = copy_in(4, nb, nb_v)
    c_fw = copy_in(5, fw, fw_v)
    c_sc = copy_in(6, sc, sc_v)
    c_de = copy_in(7, de, de_v)

    barrier = pltpu.get_barrier_semaphore()

    def greet(c, i):
        pl.semaphore_signal(barrier, inc=1, device_id={"cell": c, "inst": i}, device_id_type=MESH)

    def others(c):
        for j in range(n_inst):
            greet(c, lax.rem(inst + j, n_inst))

    partners = jnp.int32(3)
    for j in range(1, n_inst):
        greet(me, lax.rem(inst + j, n_inst))

    @pl.when(swapped)
    def _():
        greet(me, inst)

    partners = partners + jnp.where(swapped, 1, 0)
    for d in (-1, 1):
        others(mirror(wrap(cell + d)))
        others(wrap(me + d))
        partners = partners + 2 * n_inst
    for d in (-3, -2, 2, 3):
        for target in (mirror(wrap(cell + d)), wrap(me - d)):
            @pl.when(target != cell)
            def _():
                greet(target, inst)

            partners = partners + jnp.where(target != cell, 1, 0)
    for d in OFFSETS:
        greet(mirror(wrap(me + d)), inst)
        partners = partners + 1

    c_rt.wait()
    group = lax.broadcasted_iota(jnp.int32, (8, BLK), 0) * 8 + lax.broadcasted_iota(jnp.int32, (8, BLK), 1) // CB

    above = wrap(cell + 1)

    def find(step, carry):
        c0, c1, inv, fwd = carry
        for u in range(8):
            b = step * 8 + u
            route = rt_s[0, b]
            is0 = route == above
            is1 = route == cell
            pos = jnp.where(is1, c1, jnp.where(is0, c0, blocks + b - c0 - c1))
            c0 = c0 + jnp.where(is0, 1, 0)
            c1 = c1 + jnp.where(is1, 1, 0)
            inv = jnp.where(group == pos, b, inv)
            fwd = jnp.where(group == b, pos, fwd)
        return c0, c1, inv, fwd

    zero8 = jnp.zeros((8, BLK), jnp.int32)
    found = lax.fori_loop(0, blocks // 8, find, (jnp.int32(0), jnp.int32(handed), zero8, zero8))
    within = lax.rem(lax.broadcasted_iota(jnp.int32, (8, BLK), 1), CB)
    inv_v[...] = found[2] * CB + within
    pos_v[...] = found[3] * CB + within

    row16 = lax.broadcasted_iota(jnp.int32, (16, BLK), 0).astype(F32).astype(BF16)

    def permutation_tile(src, dst, tile):
        line = jnp.broadcast_to(src[pl.ds(tile, 1), :], (16, BLK))
        lanes = pl.ds(pl.multiple_of(tile * BLK, BLK), BLK)
        high = (line // 256).astype(F32).astype(BF16)
        low = lax.rem(line, 256).astype(F32).astype(BF16)
        for kt in range(cc // 256):
            at = jnp.where(high == jnp.asarray(kt, BF16), low, jnp.full_like(low, -1.0))
            for j in range(16):
                hit = at == row16 + jnp.asarray(16.0 * j, BF16)
                dst[256 * kt + 16 * j : 256 * kt + 16 * j + 16, lanes] = jnp.where(
                    hit, jnp.ones((16, BLK), BF16), jnp.zeros((16, BLK), BF16)
                )

    c_fr.wait()
    c_fm.wait()
    kept = 2 * inst + 1 < HB_INST
    rows_of = lax.rem(lax.broadcasted_iota(jnp.int32, (BLK, BLK), 0), CB)
    block_of = lax.broadcasted_iota(jnp.int32, (16, BLK), 0) // 2 == lax.broadcasted_iota(jnp.int32, (16, BLK), 1) // CB
    drop = (lax.rem(lax.broadcasted_iota(jnp.int32, (2, BLK), 0), 2) == 0) | kept

    def restrict(tile):
        maps = [jnp.broadcast_to(fm_v[pl.ds(tile * 8 + e, 1), :], (CB, BLK)) for e in range(8)]
        onehot = jnp.where(rows_of == jnp.concatenate(maps, axis=0), 1.0, 0.0).astype(BF16)
        rows = pl.ds(pl.multiple_of(tile * 16, 16), 16)
        lanes = pl.ds(pl.multiple_of(tile * BLK, BLK), BLK)
        his, los = [], []
        for v in range(VARS):
            hi, lo = split2(fr_v[v, rows, :])
            his.append(hi)
            los.append(lo)
        got = dot_t(jnp.concatenate(his + los, axis=0), onehot)
        for v in range(VARS):
            both = jnp.where(block_of, got[16 * v : 16 * v + 16] + got[96 + 16 * v : 112 + 16 * v], 0.0)
            half = both[0:8] + both[8:16]
            half = half[0:4] + half[4:8]
            yu[v // 2, 2 * (v % 2) : 2 * (v % 2) + 2, lanes] = jnp.where(drop, half[0:2] + half[2:4], 0.0)

    def restrict_some(step, _):
        for u in range(4):
            restrict(step * 4 + u)
            permutation_tile(inv_v, perm, step * 4 + u)
        return 0

    lax.fori_loop(0, cc // BLK // 4, restrict_some, 0)
    terms = split3(jnp.concatenate([yu[0], yu[1], yu[2], yu[2]], axis=0))
    terms = jnp.concatenate(terms, axis=0)
    for nt in (0, cc // 256 - 1, *range(1, cc // 256 - 1)):
        got = dot(terms, perm[:, 256 * nt : 256 * nt + 256])
        got = got[0:16] + got[16:32] + got[32:48]
        for g in range(SWEEPERS):
            ysend[g, :, 256 * nt : 256 * nt + 256] = got[4 * g : 4 * g + 4, :]

    c_rl.wait()
    lsend[...] = jnp.zeros_like(lsend)
    lsend[:, : PEERS * HS] = rl_v[...]

    c_nb.wait()
    c_fw.wait()
    c_sc.wait()
    c_de.wait()
    total = fw_v[0:1, :]
    for s in range(1, NB):
        total = total + fw_v[s : s + 1, :]
    total = total + 3.0 * sc_v[...]
    for v in range(2):
        extra = jnp.where(
            inst == 0, de_v[v : v + 1, :], jnp.where(inst == 1, de_v[2 + v : 3 + v, :], de_v[4 + v : 5 + v, :])
        )
        dsend[v : v + 1, :] = total + extra
    dsend[2:3, :] = sc_v[...]
    dsend[3:4, :] = sc_v[...]

    pl.semaphore_wait(barrier, partners)

    def taken_all(ref, sem):
        pltpu.make_async_copy(ref, ref, sem).wait()

    def list_copy(t):
        return pltpu.make_async_remote_copy(
            src_ref=lsend, dst_ref=lrx.at[t], send_sem=out_sem.at[0], recv_sem=list_sem.at[0],
            device_id={"cell": mirror(wrap(cell + OFFSETS[t])), "inst": inst}, device_id_type=MESH,
        )

    moves = ((dsend, drx), (nb_v, nb_r), (fw_v, fw_r))

    def move_copy(m):
        return pltpu.make_async_remote_copy(
            src_ref=moves[m][0], dst_ref=moves[m][1], send_sem=out_sem.at[6 + m], recv_sem=move_sem.at[m],
            device_id={"cell": me, "inst": inst}, device_id_type=MESH,
        )

    def move(m):
        @pl.when(swapped)
        def _():
            move_copy(m).start()

        @pl.when(jnp.logical_not(swapped))
        def _():
            pltpu.make_async_copy(*moves[m], move_sem.at[m]).start()

    def rest_copy(g, kind):
        if kind == 0:
            src, dst = ysend.at[g], rx.at[inst]
        else:
            src = ysend.at[g, :, pl.ds((0, cc - BLK)[kind - 1], BLK)]
            dst = rxe.at[kind - 1, inst]
        return pltpu.make_async_remote_copy(
            src_ref=src, dst_ref=dst, send_sem=out_sem.at[1 + min(kind, 1)], recv_sem=rest_sem.at[min(kind, 1)],
            device_id={"cell": mirror(wrap(cell + (0, 1, -1)[kind])), "inst": g}, device_id_type=MESH,
        )

    def halo_copy(k, t):
        return pltpu.make_async_remote_copy(
            src_ref=xsend.at[k, t // 4], dst_ref=halo.at[k, t], send_sem=out_sem.at[3], recv_sem=halo_sem.at[k],
            device_id={"cell": mirror(wrap(me - OFFSETS[t])), "inst": inst}, device_id_type=MESH,
        )

    def back_copy(g, kind):
        if kind == 0:
            src, dst = xf.at[g], gx.at[inst]
        else:
            src = xf.at[g, :, pl.ds((0, cc - BLK)[kind - 1], BLK)]
            dst = gxe.at[kind - 1, inst]
        return pltpu.make_async_remote_copy(
            src_ref=src, dst_ref=dst, send_sem=out_sem.at[4 + min(kind, 1)], recv_sem=back_sem.at[min(kind, 1)],
            device_id={"cell": wrap(me + (0, -1, 1)[kind]), "inst": g}, device_id_type=MESH,
        )

    sweeping = inst < SWEEPERS

    @pl.when(sweeping)
    def _():
        for t in range(PEERS):
            if abs(OFFSETS[t]) == 2:
                here = mirror(wrap(cell + OFFSETS[t])) == cell

                @pl.when(here)
                def _():
                    pltpu.make_async_copy(lsend, lrx.at[t], list_sem.at[0]).start()

                @pl.when(jnp.logical_not(here))
                def _():
                    list_copy(t).start()
            else:
                list_copy(t).start()

    for kind in (1, 2):
        for g in range(SWEEPERS):
            rest_copy(g, kind).start()

    @pl.when(sweeping)
    def _():
        move(0)

    for g in range(SWEEPERS):
        local = (inst == g) & jnp.logical_not(swapped)

        @pl.when(jnp.logical_not(local))
        def _():
            rest_copy(g, 0).start()

        @pl.when(local)
        def _():
            pltpu.make_async_copy(ysend.at[g], rx.at[g], rest_sem.at[0]).start()

    @pl.when(sweeping)
    def _():
        move(1)
        move(2)

    row = lax.broadcasted_iota(jnp.int32, (ROWS, BLK), 0)
    row_n = 2 * (row // 4) + row % 2
    row_v = (row % 4) // 2
    live = [p for p in range(ROWS) if 2 * (p // 4) + p % 2 < HB_INST]
    for slot, p in enumerate(live):
        n, v = 2 * (p // 4) + p % 2, (p % 4) // 2
        value = jnp.zeros((ROWS, BLK), F32)
        for m in range(HB_INST):
            value = jnp.where((row_n == m) & (row_v == v), spectral_value(m - n), value)
        coef[slot] = value

    quarter = lax.broadcasted_iota(jnp.int32, (ROWS, BLK), 1) // HS

    def build(src, lane_tiles, first_tile):
        def one(m, _):
            lt, kt = m // 5, lax.rem(m, 5)
            s_lanes = pl.ds(pl.multiple_of(lt * BLK, BLK), BLK)
            d_lanes = pl.ds(pl.multiple_of((lt + first_tile) * BLK, BLK), BLK)
            kf = kt.astype(F32).astype(BF16)
            at = []
            def line(i):
                return jnp.broadcast_to(src[i : i + 1, s_lanes], (16, BLK)).astype(BF16)

            for s in range(NB):
                r = line(T_R + s)
                at.append(jnp.where(line(T_Q + s) == kf, r, jnp.full_like(r, -1.0)))
            hs = [line(T_H + s) for s in range(NB)]
            ls = [line(T_L + s) for s in range(NB)]
            for j in range(16):
                here = row16 + jnp.asarray(16.0 * j, BF16)
                h = jnp.zeros((16, BLK), BF16)
                low = jnp.zeros((16, BLK), BF16)
                for s in range(NB):
                    hit = at[s] == here
                    h = jnp.where(hit, hs[s], h)
                    low = jnp.where(hit, ls[s], low)
                k_rows = pl.ds(pl.multiple_of(kt * 256 + 16 * j, 16), 16)
                wh[k_rows, d_lanes] = h
                wl[k_rows, d_lanes] = low
            return 0

        lax.fori_loop(*(5 * tile for tile in lane_tiles), one, 0)

    tiles = (SEND + cc) // 256

    def keep(x_all):
        own_hi, own_lo = split2(x_all[:, SEND:])
        xh_v[0:16, :] = own_hi
        xh_v[16:32, :] = own_lo
        x_v[...] = x_all

    def local_part(which):
        for nt in which:
            lanes = pl.ds(256 * nt, 256)
            a = dot(xh_v[...], wh[0:cc, lanes])
            b = dot(xh_v[0:16, :], wl[0:cc, lanes])
            halves = []
            for e in range(2):
                part = pl.ds(256 * nt + 128 * e, 128)
                acc = jnp.zeros((ROWS, BLK), F32)
                for slot, p in enumerate(live):
                    acc = acc + coef[slot] * jnp.broadcast_to(x_v[p : p + 1, part], (ROWS, BLK))
                halves.append(acc)
            sx = jnp.concatenate(halves, axis=1)
            base_v[:, lanes] = r_v[:, lanes] - sg_v[:, lanes] * sx + (a[0:16] + a[16:32] + b)

    def halo_rows(k):
        taken_all(halo.at[k], halo_sem.at[k])
        first = halo[k, 0]
        for t in range(1, 4):
            first = jnp.where(quarter == t, halo[k, t], first)
        second = jnp.where(quarter == 0, halo[k, 4], jnp.where(quarter == 1, halo[k, 5], 0.0))
        hi, lo = split2(jnp.concatenate([first, second], axis=1))
        return jnp.concatenate([hi, lo], axis=0)

    def with_halo(rows, lanes):
        a = dot(rows, wh[cc : cc + 256, lanes])
        b = dot(rows[0:16], wl[cc : cc + 256, lanes])
        return (base_v[:, lanes] + (a[0:16] + a[16:32] + b)) * di_v[:, lanes]

    def send_halo(k, x_send):
        xsend[k, 0] = x_send[:, 0:BLK]
        xsend[k, 1] = x_send[:, BLK:SEND]
        for t in range(PEERS):
            halo_copy(k, t).start()

    @pl.when(sweeping)
    def _():
        def own_table():
            taken_all(nb_r, move_sem.at[1])
            taken_all(fw_r, move_sem.at[2])
            ids = [jnp.broadcast_to(nb_r[s : s + 1, :], (8, cc)) for s in range(NB)]
            face = [jnp.broadcast_to(fw_r[s : s + 1, :], (8, cc)) for s in range(NB)]
            for s in range(NB):
                for o in range(s + 1, NB):
                    same = ids[s] == ids[o]
                    face[s] = face[s] + jnp.where(same, face[o], 0.0)
                    ids[o] = jnp.where(same, 2047, ids[o])
            for s in range(NB):
                table[T_Q + s : T_Q + s + 1, :] = lax.shift_right_logical(ids[s], 8).astype(F32)[0:1]
                table[T_R + s : T_R + s + 1, :] = (ids[s] & 255).astype(F32)[0:1]
                hi = face[s].astype(BF16).astype(F32)
                table[T_H + s : T_H + s + 1, :] = hi[0:1]
                table[T_L + s : T_L + s + 1, :] = (face[s] - hi).astype(BF16).astype(F32)[0:1]

        @pl.when(jnp.logical_not(swapped))
        def _():
            own_table()
            build(table, (0, EARLY), SEND // BLK)

        taken_all(lrx, list_sem.at[0])
        lane_slot = lax.broadcasted_iota(jnp.int32, (1, SEND), 1) // HS
        wanted = jnp.full((1, SEND), 4096, jnp.int32)
        for t in range(PEERS):
            wanted = jnp.where(lane_slot == t, lrx[t], wanted)
        for kt in range(cc // 256):
            rows256 = lax.broadcasted_iota(jnp.int32, (256, SEND), 0) + 256 * kt
            sel[256 * kt : 256 * kt + 256, :] = jnp.where(rows256 == wanted, 1.0, 0.0).astype(BF16)
        taken_all(drx, move_sem.at[0])
        late = dot(jnp.concatenate(split3(jnp.concatenate([drx[...], drx[...]], axis=0)), axis=0), sel[...])
        late = late[0:8] + late[8:16] + late[16:24]

        def by_variable(x, width):
            second = lax.rem(lax.broadcasted_iota(jnp.int32, (ROWS, width), 0), 4) >= 2
            return jnp.where(second, jnp.broadcast_to(x[1:2], (ROWS, width)), jnp.broadcast_to(x[0:1], (ROWS, width)))

        used = lane_slot < PEERS
        sg_v[:, 0:SEND] = jnp.broadcast_to(late[2:3], (ROWS, SEND))
        di_v[:, 0:SEND] = 1.0 / jnp.where(used, by_variable(late, SEND), 1.0)
        sg_v[:, SEND:] = jnp.broadcast_to(drx[2:3, :], (ROWS, cc))
        di_v[:, SEND:] = 1.0 / by_variable(drx[...], cc)
        taken_all(rxe, rest_sem.at[1])
        taken_all(rx, rest_sem.at[0])
        lane = lax.broadcasted_iota(jnp.int32, (ROWS, BLK), 1)
        mine = jnp.concatenate([rx[src] for src in range(n_inst)], axis=0)
        low = jnp.concatenate([rxe[0, src] for src in range(n_inst)], axis=0)
        high = jnp.concatenate([rxe[1, src] for src in range(n_inst)], axis=0)
        edge = handed * CB
        rest = jnp.concatenate(
            [
                jnp.where(lane < edge, low, mine[:, 0:BLK]),
                mine[:, BLK : cc - BLK],
                jnp.where(lane >= BLK - edge, high, mine[:, cc - BLK :]),
            ],
            axis=1,
        )
        parts = dot(jnp.concatenate(split3(rest), axis=0), sel[...])
        r_send = parts[0:16] + parts[16:32] + parts[32:48]
        x_send = r_send * di_v[:, 0:SEND]
        send_halo(0, x_send)
        r_v[:, 0:SEND] = r_send
        r_v[:, SEND:] = rest
        keep(jnp.concatenate([x_send, rest * di_v[:, SEND:]], axis=1))

        @pl.when(swapped)
        def _():
            own_table()

        stable[...] = dot(table[...].astype(BF16), sel[...])
        build(stable, (0, SEND // BLK), 0)
        local_part((0,))

        def own_sweep(rows, x_send):
            local_part(range(1, tiles))
            parts = [x_send]
            for nt in range(cc // 256):
                parts.append(with_halo(rows, pl.ds(SEND + 256 * nt, 256)))
            keep(jnp.concatenate(parts, axis=1))
            local_part((0,))

        rows = halo_rows(0)
        x_send = with_halo(rows, pl.ds(0, SEND))
        send_halo(1, x_send)
        build(table, (jnp.where(swapped, 0, EARLY), cc // BLK), SEND // BLK)
        own_sweep(rows, x_send)

        def sweep(k, _):
            rows = halo_rows(k)
            x_send = with_halo(rows, pl.ds(0, SEND))
            send_halo(k + 1, x_send)
            own_sweep(rows, x_send)
            return 0

        lax.fori_loop(1, ITERS - 1, sweep, 0)
        local_part(range(1, tiles))
        rows = halo_rows(ITERS - 1)
        for nt in (0, cc // 256 - 1, *range(1, cc // 256 - 1)):
            out = with_halo(rows, pl.ds(SEND + 256 * nt, 256))
            for g in range(n_inst):
                xf[g, :, 256 * nt : 256 * nt + 256] = out[4 * g : 4 * g + 4, :]
            if nt == cc // 256 - 1:
                for kind in (1, 2):
                    for g in range(n_inst):
                        back_copy(g, kind).start()
        for g in range(n_inst):
            local = (inst == g) & jnp.logical_not(swapped)

            @pl.when(jnp.logical_not(local))
            def _():
                back_copy(g, 0).start()

            if g < SWEEPERS:
                @pl.when(local)
                def _():
                    pltpu.make_async_copy(xf.at[g], gx.at[g], back_sem.at[0]).start()

    def permute_back(step, _):
        for u in range(2):
            permutation_tile(pos_v, perm_t, step * 2 + u)
        return 0

    lax.fori_loop(0, cc // BLK // 2, permute_back, 0)
    taken_all(gxe, back_sem.at[1])
    taken_all(gx, back_sem.at[0])
    lane4 = lax.broadcasted_iota(jnp.int32, (4, BLK), 1)
    edge = handed * CB
    placed = []
    for src in range(SWEEPERS):
        own = gx[src]
        first = jnp.where(lane4 < edge, gxe[0, src], own[:, 0:BLK])
        last = jnp.where(lane4 >= BLK - edge, gxe[1, src], own[:, cc - BLK :])
        coarse_o[src] = own
        placed.append(jnp.concatenate([first, own[:, BLK : cc - BLK], last], axis=1))
    terms = jnp.concatenate(split3(jnp.concatenate(placed + placed[2:], axis=0)), axis=0)
    for nt in range(cc // 256):
        got = dot(terms, perm_t[:, 256 * nt : 256 * nt + 256])
        got = got[0:16] + got[16:32] + got[32:48]
        for g in range(SWEEPERS):
            blocks_o[g, :, 256 * nt : 256 * nt + 256] = got[4 * g : 4 * g + 4, :]

    taken_all(ysend.at[:, :, 0:256], out_sem.at[2])

    @pl.when(sweeping & jnp.logical_not(swapped))
    def _():
        taken_all(ysend.at[0 : SWEEPERS - 1], out_sem.at[1])
        taken_all(xf.at[0 : n_inst - 1], out_sem.at[4])

    @pl.when(jnp.logical_not(sweeping) | swapped)
    def _():
        taken_all(ysend, out_sem.at[1])

    @pl.when(sweeping & swapped)
    def _():
        taken_all(xf, out_sem.at[4])
        for m in range(3):
            taken_all(moves[m][1], out_sem.at[6 + m])

    @pl.when(sweeping)
    def _():
        at_home = (mirror(wrap(cell + 2)) == cell) | (mirror(wrap(cell - 2)) == cell)

        @pl.when(at_home)
        def _():
            taken_all(lrx.at[0 : PEERS - 1], out_sem.at[0])

        @pl.when(jnp.logical_not(at_home))
        def _():
            taken_all(lrx, out_sem.at[0])

        taken_all(halo, out_sem.at[3])
        taken_all(xf.at[:, :, 0:256], out_sem.at[5])


def prolong(fm, coarse, blocks_x, fine_o, coarse_o):
    for v in range(VARS):
        coarse_o[v] = coarse[v // 2, 2 * (v % 2) : 2 * (v % 2) + 2, :]
    for tile in range(blocks_x.shape[2] // BLK):
        lanes = pl.ds(tile * BLK, BLK)
        for half in range(2):
            maps = [
                jnp.broadcast_to(fm[tile * 8 + 4 * half + e : tile * 8 + 4 * half + e + 1, :], (2, BLK)) + (4 * half + e) * CB
                for e in range(4)
            ]
            index = jnp.concatenate(maps, axis=0)
            rows = pl.ds(16 * tile + 8 * half, 8)
            for v in range(VARS):
                x = blocks_x[v // 2, 2 * (v % 2) : 2 * (v % 2) + 2, lanes]
                x = jnp.concatenate([x, x, x, x], axis=0)
                fine_o[v, rows, :] = jnp.take_along_axis(x, index, axis=1, mode="promise_in_bounds")


def body(n_cell, fine_residual, fine_map, routes, receive_lists, neighbours, face_weights, spectral_coef, diag_extra):
    inst_dev, var_count, fine_dev = fine_residual.shape
    blocks = fine_dev // BLK
    cc = blocks * CB
    lanes = SEND + cc
    vmem = pltpu.VMEM
    dma = pltpu.SemaphoreType.DMA
    any_spec = pl.BlockSpec(memory_space=pl.ANY)
    out_spec = pl.BlockSpec(memory_space=pltpu.VMEM)
    fine_rows = fine_residual.reshape(inst_dev, var_count, blocks, BLK).transpose(1, 2, 0, 3)
    fine_rows = fine_rows.reshape(var_count, blocks * inst_dev, BLK)
    cells_map = fine_map.reshape(blocks, BLK)
    coarse, in_blocks = pl.pallas_call(
        functools.partial(kernel, n_cell),
        out_shape=(
            pltpu.VMEM((SWEEPERS, 4, cc), F32),
            pltpu.VMEM((SWEEPERS, 4, cc), F32),
        ),
        in_specs=[any_spec] * 8,
        out_specs=(out_spec, out_spec),
        scratch_shapes=[
            vmem(fine_rows.shape, F32),
            vmem((blocks, BLK), jnp.int32),
            pltpu.SMEM((1, blocks), jnp.int32),
            vmem((1, PEERS * HS), jnp.int32),
            vmem((NB, cc), jnp.int32),
            vmem((NB, cc), F32),
            vmem((1, cc), F32),
            vmem((VARS, cc), F32),
            vmem((8, BLK), jnp.int32),
            vmem((8, BLK), jnp.int32),
            vmem((cc, cc), BF16),
            vmem((cc, cc), BF16),
            vmem((SWEEPERS, 4, cc), F32),
            vmem((SWEEPERS, 4, cc), F32),
            vmem((4, 4, cc), F32),
            vmem((2, 4, 4, BLK), F32),
            vmem((1, SEND), jnp.int32),
            vmem((PEERS, 1, SEND), jnp.int32),
            vmem((4, cc), F32),
            vmem((4, cc), F32),
            vmem((NB, cc), jnp.int32),
            vmem((NB, cc), F32),
            vmem((T_END, cc), F32),
            vmem((T_END, SEND), F32),
            vmem((cc, SEND), BF16),
            vmem((cc + 256, lanes), BF16),
            vmem((cc + 256, lanes), BF16),
            vmem((2 * HB_INST, ROWS, BLK), F32),
            vmem((ROWS, lanes), F32),
            vmem((ROWS, lanes), F32),
            vmem((ROWS, lanes), F32),
            vmem((ROWS, lanes), F32),
            vmem((ROWS, lanes), F32),
            vmem((2 * ROWS, cc), BF16),
            vmem((ITERS, 2, ROWS, BLK), F32),
            vmem((ITERS, PEERS, ROWS, BLK), F32),
            vmem((4, 4, cc), F32),
            vmem((SWEEPERS, 4, cc), F32),
            vmem((2, SWEEPERS, 4, BLK), F32),
            dma((8,)),
            dma((9,)),
            dma((1,)),
            dma((3,)),
            dma((2,)),
            dma((ITERS,)),
            dma((2,)),
        ],
        compiler_params=pltpu.CompilerParams(collective_id=0, has_side_effects=True),
        name="multigrid",
    )(
        fine_rows,
        cells_map,
        routes,
        receive_lists,
        neighbours,
        face_weights,
        spectral_coef.reshape(1, cc),
        diag_extra,
    )
    fine, coarse = pl.pallas_call(
        prolong,
        out_shape=(
            jax.ShapeDtypeStruct(fine_rows.shape, F32),
            jax.ShapeDtypeStruct((var_count, inst_dev, cc), F32),
        ),
        in_specs=[out_spec] * 3,
        out_specs=(out_spec, out_spec),
        compiler_params=pltpu.CompilerParams(vmem_limit_bytes=8 << 20),
        name="prolong",
    )(
        cells_map,
        pltpu.with_memory_space_constraint(coarse, pltpu.VMEM),
        pltpu.with_memory_space_constraint(in_blocks, pltpu.VMEM),
    )
    fine = fine.reshape(var_count, blocks, inst_dev, BLK).transpose(2, 0, 1, 3).reshape(inst_dev, var_count, fine_dev)
    return fine, coarse.transpose(1, 0, 2)


def solution(mesh):
    in_specs = (
        P("inst", None, "cell"),
        P("cell"),
        P("cell", None),
        P("cell", None),
        P(None, "cell"),
        P(None, "cell"),
        P("cell"),
        P(None, "cell"),
    )
    out_specs = (P("inst", None, "cell"), P("inst", None, "cell"))
    return jax.shard_map(
        functools.partial(body, mesh.shape["cell"]), mesh=mesh, in_specs=in_specs, out_specs=out_specs, check_vma=False
    )
```

```python
import functools
import math

import jax
import jax.numpy as jnp
from jax import lax
from jax.experimental import pallas as pl
from jax.experimental.pallas import tpu as pltpu
from jax.sharding import PartitionSpec as P

INST = 8
HB_INST = 7
VARS = 6
NB = 6
BLK = 128
CB = 16
RAD = 3
HS = 32
ITERS = 6
PEERS = 2 * RAD
OFFSETS = [t - RAD if t < RAD else t - RAD + 1 for t in range(PEERS)]
SWEEPERS = 3
ROWS = 16
SEND = 256
MESH = pl.DeviceIdType.MESH
F32 = jnp.float32
BF16 = jnp.bfloat16
T_Q, T_R, T_H, T_L, T_END = 0, 6, 12, 18, 24
PLANE, CORES = 8, 2
EARLY = 5


def spectral_value(distance):
    if distance == 0:
        return 0.0
    sign = -1.0 if distance % 2 else 1.0
    return 0.5 * sign / math.sin(math.pi * distance / HB_INST)


def split2(x):
    hi = x.astype(BF16)
    return hi, (x - hi.astype(F32)).astype(BF16)


def split3(x):
    hi = x.astype(BF16)
    rest = x - hi.astype(F32)
    mid = rest.astype(BF16)
    return hi, mid, (rest - mid.astype(F32)).astype(BF16)


def dot(a, b):
    return lax.dot_general(a, b, (((1,), (0,)), ((), ())), preferred_element_type=F32)


def dot_t(a, b):
    return lax.dot_general(a, b, (((1,), (1,)), ((), ())), preferred_element_type=F32)


def kernel(
    n_cell,
    fr, fm, rt, rl, nb, fw, sc, de,
    coarse_o, blocks_o,
    fr_v, fm_v, rt_s, rl_v, nb_v, fw_v, sc_v, de_v,
    inv_v, pos_v, perm, perm_t, yu,
    ysend, rx, rxe, lsend, lrx, dsend, drx, nb_r, fw_r,
    table, stable, sel, wh, wl, coef,
    r_v, sg_v, di_v, base_v, x_v, xh_v,
    xsend, halo, xf, gx, gxe,
    in_sem, out_sem, list_sem, move_sem, rest_sem, halo_sem, back_sem,
):
    cell = lax.axis_index("cell")
    inst = lax.axis_index("inst")
    blocks = fm_v.shape[0]
    handed = blocks // 16
    cc = blocks * CB
    n_inst = 4

    def wrap(c):
        return lax.rem(c + n_cell, n_cell)

    def mirror(c):
        z, place = lax.div(c, PLANE), lax.rem(c, PLANE)
        core = lax.rem(place, CORES)
        return jnp.where(lax.rem(z, 2) == 1, z * PLANE + (PLANE - CORES) - (place - core) + core, c)

    me = mirror(cell)
    swapped = me != cell

    def copy_in(i, src, dst):
        c = pltpu.make_async_copy(src, dst, in_sem.at[i])
        c.start()
        return c

    c_rt = copy_in(0, rt, rt_s)
    c_fr = copy_in(1, fr, fr_v)
    c_fm = copy_in(2, fm, fm_v)
    c_rl = copy_in(3, rl, rl_v)
    c_nb = copy_in(4, nb, nb_v)
    c_fw = copy_in(5, fw, fw_v)
    c_sc = copy_in(6, sc, sc_v)
    c_de = copy_in(7, de, de_v)

    barrier = pltpu.get_barrier_semaphore()

    def greet(c, i):
        pl.semaphore_signal(barrier, inc=1, device_id={"cell": c, "inst": i}, device_id_type=MESH)

    def others(c):
        for j in range(n_inst):
            greet(c, lax.rem(inst + j, n_inst))

    partners = jnp.int32(3)
    for j in range(1, n_inst):
        greet(me, lax.rem(inst + j, n_inst))

    @pl.when(swapped)
    def _():
        greet(me, inst)

    partners = partners + jnp.where(swapped, 1, 0)
    for d in (-1, 1):
        others(mirror(wrap(cell + d)))
        others(wrap(me + d))
        partners = partners + 2 * n_inst
    for d in (-3, -2, 2, 3):
        for target in (mirror(wrap(cell + d)), wrap(me - d)):
            @pl.when(target != cell)
            def _():
                greet(target, inst)

            partners = partners + jnp.where(target != cell, 1, 0)
    for d in OFFSETS:
        greet(mirror(wrap(me + d)), inst)
        partners = partners + 1

    c_rt.wait()
    group = lax.broadcasted_iota(jnp.int32, (8, BLK), 0) * 8 + lax.broadcasted_iota(jnp.int32, (8, BLK), 1) // CB

    above = wrap(cell + 1)

    def find(step, carry):
        c0, c1, inv, fwd = carry
        for u in range(8):
            b = step * 8 + u
            route = rt_s[0, b]
            is0 = route == above
            is1 = route == cell
            pos = jnp.where(is1, c1, jnp.where(is0, c0, blocks + b - c0 - c1))
            c0 = c0 + jnp.where(is0, 1, 0)
            c1 = c1 + jnp.where(is1, 1, 0)
            inv = jnp.where(group == pos, b, inv)
            fwd = jnp.where(group == b, pos, fwd)
        return c0, c1, inv, fwd

    zero8 = jnp.zeros((8, BLK), jnp.int32)
    found = lax.fori_loop(0, blocks // 8, find, (jnp.int32(0), jnp.int32(handed), zero8, zero8))
    within = lax.rem(lax.broadcasted_iota(jnp.int32, (8, BLK), 1), CB)
    inv_v[...] = found[2] * CB + within
    pos_v[...] = found[3] * CB + within

    row16 = lax.broadcasted_iota(jnp.int32, (16, BLK), 0).astype(F32).astype(BF16)

    def permutation_tile(src, dst, tile):
        line = jnp.broadcast_to(src[pl.ds(tile, 1), :], (16, BLK))
        lanes = pl.ds(pl.multiple_of(tile * BLK, BLK), BLK)
        high = (line // 256).astype(F32).astype(BF16)
        low = lax.rem(line, 256).astype(F32).astype(BF16)
        for kt in range(cc // 256):
            at = jnp.where(high == jnp.asarray(kt, BF16), low, jnp.full_like(low, -1.0))
            for j in range(16):
                hit = at == row16 + jnp.asarray(16.0 * j, BF16)
                dst[256 * kt + 16 * j : 256 * kt + 16 * j + 16, lanes] = jnp.where(
                    hit, jnp.ones((16, BLK), BF16), jnp.zeros((16, BLK), BF16)
                )

    c_fr.wait()
    c_fm.wait()
    kept = 2 * inst + 1 < HB_INST
    rows_of = lax.rem(lax.broadcasted_iota(jnp.int32, (BLK, BLK), 0), CB)
    block_of = lax.broadcasted_iota(jnp.int32, (16, BLK), 0) // 2 == lax.broadcasted_iota(jnp.int32, (16, BLK), 1) // CB
    drop = (lax.rem(lax.broadcasted_iota(jnp.int32, (2, BLK), 0), 2) == 0) | kept

    def restrict(tile):
        maps = [jnp.broadcast_to(fm_v[pl.ds(tile * 8 + e, 1), :], (CB, BLK)) for e in range(8)]
        onehot = jnp.where(rows_of == jnp.concatenate(maps, axis=0), 1.0, 0.0).astype(BF16)
        rows = pl.ds(pl.multiple_of(tile * 16, 16), 16)
        lanes = pl.ds(pl.multiple_of(tile * BLK, BLK), BLK)
        his, los = [], []
        for v in range(VARS):
            hi, lo = split2(fr_v[v, rows, :])
            his.append(hi)
            los.append(lo)
        got = dot_t(jnp.concatenate(his + los, axis=0), onehot)
        for v in range(VARS):
            both = jnp.where(block_of, got[16 * v : 16 * v + 16] + got[96 + 16 * v : 112 + 16 * v], 0.0)
            half = both[0:8] + both[8:16]
            half = half[0:4] + half[4:8]
            yu[v // 2, 2 * (v % 2) : 2 * (v % 2) + 2, lanes] = jnp.where(drop, half[0:2] + half[2:4], 0.0)

    def restrict_some(step, _):
        for u in range(4):
            restrict(step * 4 + u)
            permutation_tile(inv_v, perm, step * 4 + u)
        return 0

    lax.fori_loop(0, cc // BLK // 4, restrict_some, 0)
    terms = split3(jnp.concatenate([yu[0], yu[1], yu[2], yu[2]], axis=0))
    terms = jnp.concatenate(terms, axis=0)
    for nt in (0, cc // 256 - 1, *range(1, cc // 256 - 1)):
        got = dot(terms, perm[:, 256 * nt : 256 * nt + 256])
        got = got[0:16] + got[16:32] + got[32:48]
        for g in range(SWEEPERS):
            ysend[g, :, 256 * nt : 256 * nt + 256] = got[4 * g : 4 * g + 4, :]

    c_rl.wait()
    lsend[...] = jnp.zeros_like(lsend)
    lsend[:, : PEERS * HS] = rl_v[...]

    c_nb.wait()
    c_fw.wait()
    c_sc.wait()
    c_de.wait()
    total = fw_v[0:1, :]
    for s in range(1, NB):
        total = total + fw_v[s : s + 1, :]
    total = total + 3.0 * sc_v[...]
    for v in range(2):
        extra = jnp.where(
            inst == 0, de_v[v : v + 1, :], jnp.where(inst == 1, de_v[2 + v : 3 + v, :], de_v[4 + v : 5 + v, :])
        )
        dsend[v : v + 1, :] = total + extra
    dsend[2:3, :] = sc_v[...]
    dsend[3:4, :] = sc_v[...]

    pl.semaphore_wait(barrier, partners)

    def taken_all(ref, sem):
        pltpu.make_async_copy(ref, ref, sem).wait()

    def list_copy(t):
        return pltpu.make_async_remote_copy(
            src_ref=lsend, dst_ref=lrx.at[t], send_sem=out_sem.at[0], recv_sem=list_sem.at[0],
            device_id={"cell": mirror(wrap(cell + OFFSETS[t])), "inst": inst}, device_id_type=MESH,
        )

    moves = ((dsend, drx), (nb_v, nb_r), (fw_v, fw_r))

    def move_copy(m):
        return pltpu.make_async_remote_copy(
            src_ref=moves[m][0], dst_ref=moves[m][1], send_sem=out_sem.at[6 + m], recv_sem=move_sem.at[m],
            device_id={"cell": me, "inst": inst}, device_id_type=MESH,
        )

    def move(m):
        @pl.when(swapped)
        def _():
            move_copy(m).start()

        @pl.when(jnp.logical_not(swapped))
        def _():
            pltpu.make_async_copy(*moves[m], move_sem.at[m]).start()

    def rest_copy(g, kind):
        if kind == 0:
            src, dst = ysend.at[g], rx.at[inst]
        else:
            src = ysend.at[g, :, pl.ds((0, cc - BLK)[kind - 1], BLK)]
            dst = rxe.at[kind - 1, inst]
        return pltpu.make_async_remote_copy(
            src_ref=src, dst_ref=dst, send_sem=out_sem.at[1 + min(kind, 1)], recv_sem=rest_sem.at[min(kind, 1)],
            device_id={"cell": mirror(wrap(cell + (0, 1, -1)[kind])), "inst": g}, device_id_type=MESH,
        )

    def halo_copy(k, t):
        return pltpu.make_async_remote_copy(
            src_ref=xsend.at[k, t // 4], dst_ref=halo.at[k, t], send_sem=out_sem.at[3], recv_sem=halo_sem.at[k],
            device_id={"cell": mirror(wrap(me - OFFSETS[t])), "inst": inst}, device_id_type=MESH,
        )

    def back_copy(g, kind):
        if kind == 0:
            src, dst = xf.at[g], gx.at[inst]
        else:
            src = xf.at[g, :, pl.ds((0, cc - BLK)[kind - 1], BLK)]
            dst = gxe.at[kind - 1, inst]
        return pltpu.make_async_remote_copy(
            src_ref=src, dst_ref=dst, send_sem=out_sem.at[4 + min(kind, 1)], recv_sem=back_sem.at[min(kind, 1)],
            device_id={"cell": wrap(me + (0, -1, 1)[kind]), "inst": g}, device_id_type=MESH,
        )

    sweeping = inst < SWEEPERS

    @pl.when(sweeping)
    def _():
        for t in range(PEERS):
            if abs(OFFSETS[t]) == 2:
                here = mirror(wrap(cell + OFFSETS[t])) == cell

                @pl.when(here)
                def _():
                    pltpu.make_async_copy(lsend, lrx.at[t], list_sem.at[0]).start()

                @pl.when(jnp.logical_not(here))
                def _():
                    list_copy(t).start()
            else:
                list_copy(t).start()

    for kind in (1, 2):
        for g in range(SWEEPERS):
            rest_copy(g, kind).start()

    @pl.when(sweeping)
    def _():
        move(0)

    for g in range(SWEEPERS):
        local = (inst == g) & jnp.logical_not(swapped)

        @pl.when(jnp.logical_not(local))
        def _():
            rest_copy(g, 0).start()

        @pl.when(local)
        def _():
            pltpu.make_async_copy(ysend.at[g], rx.at[g], rest_sem.at[0]).start()

    @pl.when(sweeping)
    def _():
        move(1)
        move(2)

    row = lax.broadcasted_iota(jnp.int32, (ROWS, BLK), 0)
    row_n = 2 * (row // 4) + row % 2
    row_v = (row % 4) // 2
    live = [p for p in range(ROWS) if 2 * (p // 4) + p % 2 < HB_INST]
    for slot, p in enumerate(live):
        n, v = 2 * (p // 4) + p % 2, (p % 4) // 2
        value = jnp.zeros((ROWS, BLK), F32)
        for m in range(HB_INST):
            value = jnp.where((row_n == m) & (row_v == v), spectral_value(m - n), value)
        coef[slot] = value

    quarter = lax.broadcasted_iota(jnp.int32, (ROWS, BLK), 1) // HS

    def build(src, lane_tiles, first_tile):
        def one(m, _):
            lt, kt = m // 5, lax.rem(m, 5)
            s_lanes = pl.ds(pl.multiple_of(lt * BLK, BLK), BLK)
            d_lanes = pl.ds(pl.multiple_of((lt + first_tile) * BLK, BLK), BLK)
            kf = kt.astype(F32).astype(BF16)
            at = []
            def line(i):
                return jnp.broadcast_to(src[i : i + 1, s_lanes], (16, BLK)).astype(BF16)

            for s in range(NB):
                r = line(T_R + s)
                at.append(jnp.where(line(T_Q + s) == kf, r, jnp.full_like(r, -1.0)))
            hs = [line(T_H + s) for s in range(NB)]
            ls = [line(T_L + s) for s in range(NB)]
            for j in range(16):
                here = row16 + jnp.asarray(16.0 * j, BF16)
                h = jnp.zeros((16, BLK), BF16)
                low = jnp.zeros((16, BLK), BF16)
                for s in range(NB):
                    hit = at[s] == here
                    h = jnp.where(hit, hs[s], h)
                    low = jnp.where(hit, ls[s], low)
                k_rows = pl.ds(pl.multiple_of(kt * 256 + 16 * j, 16), 16)
                wh[k_rows, d_lanes] = h
                wl[k_rows, d_lanes] = low
            return 0

        lax.fori_loop(*(5 * tile for tile in lane_tiles), one, 0)

    tiles = (SEND + cc) // 256

    def keep(x_all):
        own_hi, own_lo = split2(x_all[:, SEND:])
        xh_v[0:16, :] = own_hi
        xh_v[16:32, :] = own_lo
        x_v[...] = x_all

    def local_part(which):
        for nt in which:
            lanes = pl.ds(256 * nt, 256)
            a = dot(xh_v[...], wh[0:cc, lanes])
            b = dot(xh_v[0:16, :], wl[0:cc, lanes])
            halves = []
            for e in range(2):
                part = pl.ds(256 * nt + 128 * e, 128)
                acc = jnp.zeros((ROWS, BLK), F32)
                for slot, p in enumerate(live):
                    acc = acc + coef[slot] * jnp.broadcast_to(x_v[p : p + 1, part], (ROWS, BLK))
                halves.append(acc)
            sx = jnp.concatenate(halves, axis=1)
            base_v[:, lanes] = r_v[:, lanes] - sg_v[:, lanes] * sx + (a[0:16] + a[16:32] + b)

    def halo_rows(k):
        taken_all(halo.at[k], halo_sem.at[k])
        first = halo[k, 0]
        for t in range(1, 4):
            first = jnp.where(quarter == t, halo[k, t], first)
        second = jnp.where(quarter == 0, halo[k, 4], jnp.where(quarter == 1, halo[k, 5], 0.0))
        hi, lo = split2(jnp.concatenate([first, second], axis=1))
        return jnp.concatenate([hi, lo], axis=0)

    def with_halo(rows, lanes):
        a = dot(rows, wh[cc : cc + 256, lanes])
        b = dot(rows[0:16], wl[cc : cc + 256, lanes])
        return (base_v[:, lanes] + (a[0:16] + a[16:32] + b)) * di_v[:, lanes]

    def send_halo(k, x_send):
        xsend[k, 0] = x_send[:, 0:BLK]
        xsend[k, 1] = x_send[:, BLK:SEND]
        for t in (0, 5, 1, 4, 2, 3):
            halo_copy(k, t).start()

    @pl.when(sweeping)
    def _():
        def own_table():
            taken_all(nb_r, move_sem.at[1])
            taken_all(fw_r, move_sem.at[2])
            ids = [jnp.broadcast_to(nb_r[s : s + 1, :], (8, cc)) for s in range(NB)]
            face = [jnp.broadcast_to(fw_r[s : s + 1, :], (8, cc)) for s in range(NB)]
            for s in range(NB):
                for o in range(s + 1, NB):
                    same = ids[s] == ids[o]
                    face[s] = face[s] + jnp.where(same, face[o], 0.0)
                    ids[o] = jnp.where(same, 2047, ids[o])
            for s in range(NB):
                table[T_Q + s : T_Q + s + 1, :] = lax.shift_right_logical(ids[s], 8).astype(F32)[0:1]
                table[T_R + s : T_R + s + 1, :] = (ids[s] & 255).astype(F32)[0:1]
                hi = face[s].astype(BF16).astype(F32)
                table[T_H + s : T_H + s + 1, :] = hi[0:1]
                table[T_L + s : T_L + s + 1, :] = (face[s] - hi).astype(BF16).astype(F32)[0:1]

        @pl.when(jnp.logical_not(swapped))
        def _():
            own_table()
            build(table, (0, EARLY), SEND // BLK)

        taken_all(lrx, list_sem.at[0])
        lane_slot = lax.broadcasted_iota(jnp.int32, (1, SEND), 1) // HS
        wanted = jnp.full((1, SEND), 4096, jnp.int32)
        for t in range(PEERS):
            wanted = jnp.where(lane_slot == t, lrx[t], wanted)
        for kt in range(cc // 256):
            rows256 = lax.broadcasted_iota(jnp.int32, (256, SEND), 0) + 256 * kt
            sel[256 * kt : 256 * kt + 256, :] = jnp.where(rows256 == wanted, 1.0, 0.0).astype(BF16)
        taken_all(drx, move_sem.at[0])
        late = dot(jnp.concatenate(split3(jnp.concatenate([drx[...], drx[...]], axis=0)), axis=0), sel[...])
        late = late[0:8] + late[8:16] + late[16:24]

        def by_variable(x, width):
            second = lax.rem(lax.broadcasted_iota(jnp.int32, (ROWS, width), 0), 4) >= 2
            return jnp.where(second, jnp.broadcast_to(x[1:2], (ROWS, width)), jnp.broadcast_to(x[0:1], (ROWS, width)))

        used = lane_slot < PEERS
        sg_v[:, 0:SEND] = jnp.broadcast_to(late[2:3], (ROWS, SEND))
        di_v[:, 0:SEND] = 1.0 / jnp.where(used, by_variable(late, SEND), 1.0)
        sg_v[:, SEND:] = jnp.broadcast_to(drx[2:3, :], (ROWS, cc))
        di_v[:, SEND:] = 1.0 / by_variable(drx[...], cc)
        taken_all(rxe, rest_sem.at[1])
        taken_all(rx, rest_sem.at[0])
        lane = lax.broadcasted_iota(jnp.int32, (ROWS, BLK), 1)
        mine = jnp.concatenate([rx[src] for src in range(n_inst)], axis=0)
        low = jnp.concatenate([rxe[0, src] for src in range(n_inst)], axis=0)
        high = jnp.concatenate([rxe[1, src] for src in range(n_inst)], axis=0)
        edge = handed * CB
        rest = jnp.concatenate(
            [
                jnp.where(lane < edge, low, mine[:, 0:BLK]),
                mine[:, BLK : cc - BLK],
                jnp.where(lane >= BLK - edge, high, mine[:, cc - BLK :]),
            ],
            axis=1,
        )
        parts = dot(jnp.concatenate(split3(rest), axis=0), sel[...])
        r_send = parts[0:16] + parts[16:32] + parts[32:48]
        x_send = r_send * di_v[:, 0:SEND]
        send_halo(0, x_send)
        r_v[:, 0:SEND] = r_send
        r_v[:, SEND:] = rest
        keep(jnp.concatenate([x_send, rest * di_v[:, SEND:]], axis=1))

        @pl.when(swapped)
        def _():
            own_table()

        stable[...] = dot(table[...].astype(BF16), sel[...])
        build(stable, (0, SEND // BLK), 0)
        local_part((0,))

        def own_sweep(rows, x_send):
            local_part(range(1, tiles))
            parts = [x_send]
            for nt in range(cc // 256):
                parts.append(with_halo(rows, pl.ds(SEND + 256 * nt, 256)))
            keep(jnp.concatenate(parts, axis=1))
            local_part((0,))

        rows = halo_rows(0)
        x_send = with_halo(rows, pl.ds(0, SEND))
        send_halo(1, x_send)
        build(table, (jnp.where(swapped, 0, EARLY), cc // BLK), SEND // BLK)
        own_sweep(rows, x_send)

        def sweep(k, _):
            rows = halo_rows(k)
            x_send = with_halo(rows, pl.ds(0, SEND))
            send_halo(k + 1, x_send)
            own_sweep(rows, x_send)
            return 0

        lax.fori_loop(1, ITERS - 1, sweep, 0)
        local_part(range(1, tiles))
        rows = halo_rows(ITERS - 1)
        for nt in (0, cc // 256 - 1, *range(1, cc // 256 - 1)):
            out = with_halo(rows, pl.ds(SEND + 256 * nt, 256))
            for g in range(n_inst):
                xf[g, :, 256 * nt : 256 * nt + 256] = out[4 * g : 4 * g + 4, :]
            if nt == cc // 256 - 1:
                for kind in (1, 2):
                    for g in range(n_inst):
                        back_copy(g, kind).start()
        for g in range(n_inst):
            local = (inst == g) & jnp.logical_not(swapped)

            @pl.when(jnp.logical_not(local))
            def _():
                back_copy(g, 0).start()

            if g < SWEEPERS:
                @pl.when(local)
                def _():
                    pltpu.make_async_copy(xf.at[g], gx.at[g], back_sem.at[0]).start()

    def permute_back(step, _):
        for u in range(2):
            permutation_tile(pos_v, perm_t, step * 2 + u)
        return 0

    lax.fori_loop(0, cc // BLK // 2, permute_back, 0)
    taken_all(gxe, back_sem.at[1])
    taken_all(gx, back_sem.at[0])
    lane4 = lax.broadcasted_iota(jnp.int32, (4, BLK), 1)
    edge = handed * CB
    placed = []
    for src in range(SWEEPERS):
        own = gx[src]
        first = jnp.where(lane4 < edge, gxe[0, src], own[:, 0:BLK])
        last = jnp.where(lane4 >= BLK - edge, gxe[1, src], own[:, cc - BLK :])
        coarse_o[src] = own
        placed.append(jnp.concatenate([first, own[:, BLK : cc - BLK], last], axis=1))
    terms = jnp.concatenate(split3(jnp.concatenate(placed + placed[2:], axis=0)), axis=0)
    for nt in range(cc // 256):
        got = dot(terms, perm_t[:, 256 * nt : 256 * nt + 256])
        got = got[0:16] + got[16:32] + got[32:48]
        for g in range(SWEEPERS):
            blocks_o[g, :, 256 * nt : 256 * nt + 256] = got[4 * g : 4 * g + 4, :]

    taken_all(ysend.at[:, :, 0:256], out_sem.at[2])

    @pl.when(sweeping & jnp.logical_not(swapped))
    def _():
        taken_all(ysend.at[0 : SWEEPERS - 1], out_sem.at[1])
        taken_all(xf.at[0 : n_inst - 1], out_sem.at[4])

    @pl.when(jnp.logical_not(sweeping) | swapped)
    def _():
        taken_all(ysend, out_sem.at[1])

    @pl.when(sweeping & swapped)
    def _():
        taken_all(xf, out_sem.at[4])
        for m in range(3):
            taken_all(moves[m][1], out_sem.at[6 + m])

    @pl.when(sweeping)
    def _():
        at_home = (mirror(wrap(cell + 2)) == cell) | (mirror(wrap(cell - 2)) == cell)

        @pl.when(at_home)
        def _():
            taken_all(lrx.at[0 : PEERS - 1], out_sem.at[0])

        @pl.when(jnp.logical_not(at_home))
        def _():
            taken_all(lrx, out_sem.at[0])

        taken_all(halo, out_sem.at[3])
        taken_all(xf.at[:, :, 0:256], out_sem.at[5])


def prolong(fm, coarse, blocks_x, fine_o, coarse_o):
    for v in range(VARS):
        coarse_o[v] = coarse[v // 2, 2 * (v % 2) : 2 * (v % 2) + 2, :]
    for tile in range(blocks_x.shape[2] // BLK):
        lanes = pl.ds(tile * BLK, BLK)
        for half in range(2):
            maps = [
                jnp.broadcast_to(fm[tile * 8 + 4 * half + e : tile * 8 + 4 * half + e + 1, :], (2, BLK)) + (4 * half + e) * CB
                for e in range(4)
            ]
            index = jnp.concatenate(maps, axis=0)
            rows = pl.ds(16 * tile + 8 * half, 8)
            for v in range(VARS):
                x = blocks_x[v // 2, 2 * (v % 2) : 2 * (v % 2) + 2, lanes]
                x = jnp.concatenate([x, x, x, x], axis=0)
                fine_o[v, rows, :] = jnp.take_along_axis(x, index, axis=1, mode="promise_in_bounds")


def body(n_cell, fine_residual, fine_map, routes, receive_lists, neighbours, face_weights, spectral_coef, diag_extra):
    inst_dev, var_count, fine_dev = fine_residual.shape
    blocks = fine_dev // BLK
    cc = blocks * CB
    lanes = SEND + cc
    vmem = pltpu.VMEM
    dma = pltpu.SemaphoreType.DMA
    any_spec = pl.BlockSpec(memory_space=pl.ANY)
    out_spec = pl.BlockSpec(memory_space=pltpu.VMEM)
    fine_rows = fine_residual.reshape(inst_dev, var_count, blocks, BLK).transpose(1, 2, 0, 3)
    fine_rows = fine_rows.reshape(var_count, blocks * inst_dev, BLK)
    cells_map = fine_map.reshape(blocks, BLK)
    coarse, in_blocks = pl.pallas_call(
        functools.partial(kernel, n_cell),
        out_shape=(
            pltpu.VMEM((SWEEPERS, 4, cc), F32),
            pltpu.VMEM((SWEEPERS, 4, cc), F32),
        ),
        in_specs=[any_spec] * 8,
        out_specs=(out_spec, out_spec),
        scratch_shapes=[
            vmem(fine_rows.shape, F32),
            vmem((blocks, BLK), jnp.int32),
            pltpu.SMEM((1, blocks), jnp.int32),
            vmem((1, PEERS * HS), jnp.int32),
            vmem((NB, cc), jnp.int32),
            vmem((NB, cc), F32),
            vmem((1, cc), F32),
            vmem((VARS, cc), F32),
            vmem((8, BLK), jnp.int32),
            vmem((8, BLK), jnp.int32),
            vmem((cc, cc), BF16),
            vmem((cc, cc), BF16),
            vmem((SWEEPERS, 4, cc), F32),
            vmem((SWEEPERS, 4, cc), F32),
            vmem((4, 4, cc), F32),
            vmem((2, 4, 4, BLK), F32),
            vmem((1, SEND), jnp.int32),
            vmem((PEERS, 1, SEND), jnp.int32),
            vmem((4, cc), F32),
            vmem((4, cc), F32),
            vmem((NB, cc), jnp.int32),
            vmem((NB, cc), F32),
            vmem((T_END, cc), F32),
            vmem((T_END, SEND), F32),
            vmem((cc, SEND), BF16),
            vmem((cc + 256, lanes), BF16),
            vmem((cc + 256, lanes), BF16),
            vmem((2 * HB_INST, ROWS, BLK), F32),
            vmem((ROWS, lanes), F32),
            vmem((ROWS, lanes), F32),
            vmem((ROWS, lanes), F32),
            vmem((ROWS, lanes), F32),
            vmem((ROWS, lanes), F32),
            vmem((2 * ROWS, cc), BF16),
            vmem((ITERS, 2, ROWS, BLK), F32),
            vmem((ITERS, PEERS, ROWS, BLK), F32),
            vmem((4, 4, cc), F32),
            vmem((SWEEPERS, 4, cc), F32),
            vmem((2, SWEEPERS, 4, BLK), F32),
            dma((8,)),
            dma((9,)),
            dma((1,)),
            dma((3,)),
            dma((2,)),
            dma((ITERS,)),
            dma((2,)),
        ],
        compiler_params=pltpu.CompilerParams(collective_id=0, has_side_effects=True),
        name="multigrid",
    )(
        fine_rows,
        cells_map,
        routes,
        receive_lists,
        neighbours,
        face_weights,
        spectral_coef.reshape(1, cc),
        diag_extra,
    )
    fine, coarse = pl.pallas_call(
        prolong,
        out_shape=(
            jax.ShapeDtypeStruct(fine_rows.shape, F32),
            jax.ShapeDtypeStruct((var_count, inst_dev, cc), F32),
        ),
        in_specs=[out_spec] * 3,
        out_specs=(out_spec, out_spec),
        compiler_params=pltpu.CompilerParams(vmem_limit_bytes=8 << 20),
        name="prolong",
    )(
        cells_map,
        pltpu.with_memory_space_constraint(coarse, pltpu.VMEM),
        pltpu.with_memory_space_constraint(in_blocks, pltpu.VMEM),
    )
    fine = fine.reshape(var_count, blocks, inst_dev, BLK).transpose(2, 0, 1, 3).reshape(inst_dev, var_count, fine_dev)
    return fine, coarse.transpose(1, 0, 2)


def solution(mesh):
    in_specs = (
        P("inst", None, "cell"),
        P("cell"),
        P("cell", None),
        P("cell", None),
        P(None, "cell"),
        P(None, "cell"),
        P("cell"),
        P(None, "cell"),
    )
    out_specs = (P("inst", None, "cell"), P("inst", None, "cell"))
    return jax.shard_map(
        functools.partial(body, mesh.shape["cell"]), mesh=mesh, in_specs=in_specs, out_specs=out_specs, check_vma=False
    )
```

```python
import functools
import math

import jax
import jax.numpy as jnp
from jax import lax
from jax.experimental import pallas as pl
from jax.experimental.pallas import tpu as pltpu
from jax.sharding import PartitionSpec as P

INST = 8
HB_INST = 7
VARS = 6
NB = 6
BLK = 128
CB = 16
RAD = 3
HS = 32
ITERS = 6
PEERS = 2 * RAD
OFFSETS = [t - RAD if t < RAD else t - RAD + 1 for t in range(PEERS)]
SWEEPERS = 3
ROWS = 16
SEND = 256
MESH = pl.DeviceIdType.MESH
F32 = jnp.float32
BF16 = jnp.bfloat16
T_Q, T_R, T_H, T_L, T_END = 0, 6, 12, 18, 24
PLANE, CORES = 8, 2
EARLY = 5


def spectral_value(distance):
    if distance == 0:
        return 0.0
    sign = -1.0 if distance % 2 else 1.0
    return 0.5 * sign / math.sin(math.pi * distance / HB_INST)


def split2(x):
    hi = x.astype(BF16)
    return hi, (x - hi.astype(F32)).astype(BF16)


def split3(x):
    hi = x.astype(BF16)
    rest = x - hi.astype(F32)
    mid = rest.astype(BF16)
    return hi, mid, (rest - mid.astype(F32)).astype(BF16)


def dot(a, b):
    return lax.dot_general(a, b, (((1,), (0,)), ((), ())), preferred_element_type=F32)


def dot_t(a, b):
    return lax.dot_general(a, b, (((1,), (1,)), ((), ())), preferred_element_type=F32)


def kernel(
    n_cell,
    fr, fm, rt, rl, nb, fw, sc, de,
    coarse_o, blocks_o,
    fr_v, fm_v, rt_s, rl_v, nb_v, fw_v, sc_v, de_v,
    inv_v, pos_v, perm, perm_t, yu,
    ysend, rx, rxe, lsend, lrx, dsend, drx, nb_r, fw_r,
    table, stable, sel, wh, wl, coef,
    r_v, sg_v, di_v, base_v, x_v, xh_v,
    xsend, halo, xf, gx, gxe,
    in_sem, out_sem, list_sem, move_sem, rest_sem, halo_sem, back_sem,
):
    cell = lax.axis_index("cell")
    inst = lax.axis_index("inst")
    blocks = fm_v.shape[0]
    handed = blocks // 16
    cc = blocks * CB
    n_inst = 4

    def wrap(c):
        return lax.rem(c + n_cell, n_cell)

    def mirror(c):
        z, place = lax.div(c, PLANE), lax.rem(c, PLANE)
        core = lax.rem(place, CORES)
        return jnp.where(lax.rem(z, 2) == 1, z * PLANE + (PLANE - CORES) - (place - core) + core, c)

    me = mirror(cell)
    swapped = me != cell

    def copy_in(i, src, dst):
        c = pltpu.make_async_copy(src, dst, in_sem.at[i])
        c.start()
        return c

    c_rt = copy_in(0, rt, rt_s)
    c_fr = copy_in(1, fr, fr_v)
    c_fm = copy_in(2, fm, fm_v)
    c_rl = copy_in(3, rl, rl_v)
    c_nb = copy_in(4, nb, nb_v)
    c_fw = copy_in(5, fw, fw_v)
    c_sc = copy_in(6, sc, sc_v)
    c_de = copy_in(7, de, de_v)

    barrier = pltpu.get_barrier_semaphore()

    def greet(c, i):
        pl.semaphore_signal(barrier, inc=1, device_id={"cell": c, "inst": i}, device_id_type=MESH)

    def others(c):
        for j in range(n_inst):
            greet(c, lax.rem(inst + j, n_inst))

    partners = jnp.int32(3)
    for j in range(1, n_inst):
        greet(me, lax.rem(inst + j, n_inst))

    @pl.when(swapped)
    def _():
        greet(me, inst)

    partners = partners + jnp.where(swapped, 1, 0)
    for d in (-1, 1):
        others(mirror(wrap(cell + d)))
        others(wrap(me + d))
        partners = partners + 2 * n_inst
    for d in (-3, -2, 2, 3):
        for target in (mirror(wrap(cell + d)), wrap(me - d)):
            @pl.when(target != cell)
            def _():
                greet(target, inst)

            partners = partners + jnp.where(target != cell, 1, 0)
    for d in OFFSETS:
        greet(mirror(wrap(me + d)), inst)
        partners = partners + 1

    c_rt.wait()
    group = lax.broadcasted_iota(jnp.int32, (8, BLK), 0) * 8 + lax.broadcasted_iota(jnp.int32, (8, BLK), 1) // CB

    above = wrap(cell + 1)

    def find(step, carry):
        c0, c1, inv, fwd = carry
        for u in range(8):
            b = step * 8 + u
            route = rt_s[0, b]
            is0 = route == above
            is1 = route == cell
            pos = jnp.where(is1, c1, jnp.where(is0, c0, blocks + b - c0 - c1))
            c0 = c0 + jnp.where(is0, 1, 0)
            c1 = c1 + jnp.where(is1, 1, 0)
            inv = jnp.where(group == pos, b, inv)
            fwd = jnp.where(group == b, pos, fwd)
        return c0, c1, inv, fwd

    zero8 = jnp.zeros((8, BLK), jnp.int32)
    found = lax.fori_loop(0, blocks // 8, find, (jnp.int32(0), jnp.int32(handed), zero8, zero8))
    within = lax.rem(lax.broadcasted_iota(jnp.int32, (8, BLK), 1), CB)
    inv_v[...] = found[2] * CB + within
    pos_v[...] = found[3] * CB + within

    row16 = lax.broadcasted_iota(jnp.int32, (16, BLK), 0).astype(F32).astype(BF16)

    def permutation_tile(src, dst, tile):
        line = jnp.broadcast_to(src[pl.ds(tile, 1), :], (16, BLK))
        lanes = pl.ds(pl.multiple_of(tile * BLK, BLK), BLK)
        high = (line // 256).astype(F32).astype(BF16)
        low = lax.rem(line, 256).astype(F32).astype(BF16)
        for kt in range(cc // 256):
            at = jnp.where(high == jnp.asarray(kt, BF16), low, jnp.full_like(low, -1.0))
            for j in range(16):
                hit = at == row16 + jnp.asarray(16.0 * j, BF16)
                dst[256 * kt + 16 * j : 256 * kt + 16 * j + 16, lanes] = jnp.where(
                    hit, jnp.ones((16, BLK), BF16), jnp.zeros((16, BLK), BF16)
                )

    c_fr.wait()
    c_fm.wait()
    kept = 2 * inst + 1 < HB_INST
    rows_of = lax.rem(lax.broadcasted_iota(jnp.int32, (BLK, BLK), 0), CB)
    block_of = lax.broadcasted_iota(jnp.int32, (16, BLK), 0) // 2 == lax.broadcasted_iota(jnp.int32, (16, BLK), 1) // CB
    drop = (lax.rem(lax.broadcasted_iota(jnp.int32, (2, BLK), 0), 2) == 0) | kept

    def restrict(tile):
        maps = [jnp.broadcast_to(fm_v[pl.ds(tile * 8 + e, 1), :], (CB, BLK)) for e in range(8)]
        onehot = jnp.where(rows_of == jnp.concatenate(maps, axis=0), 1.0, 0.0).astype(BF16)
        rows = pl.ds(pl.multiple_of(tile * 16, 16), 16)
        lanes = pl.ds(pl.multiple_of(tile * BLK, BLK), BLK)
        his, los = [], []
        for v in range(VARS):
            hi, lo = split2(fr_v[v, rows, :])
            his.append(hi)
            los.append(lo)
        got = dot_t(jnp.concatenate(his + los, axis=0), onehot)
        for v in range(VARS):
            both = jnp.where(block_of, got[16 * v : 16 * v + 16] + got[96 + 16 * v : 112 + 16 * v], 0.0)
            half = both[0:8] + both[8:16]
            half = half[0:4] + half[4:8]
            yu[v // 2, 2 * (v % 2) : 2 * (v % 2) + 2, lanes] = jnp.where(drop, half[0:2] + half[2:4], 0.0)

    def restrict_some(step, _):
        for u in range(4):
            restrict(step * 4 + u)
            permutation_tile(inv_v, perm, step * 4 + u)
        return 0

    lax.fori_loop(0, cc // BLK // 4, restrict_some, 0)
    terms = split3(jnp.concatenate([yu[0], yu[1], yu[2], yu[2]], axis=0))
    terms = jnp.concatenate(terms, axis=0)
    for nt in (0, cc // 256 - 1, *range(1, cc // 256 - 1)):
        got = dot(terms, perm[:, 256 * nt : 256 * nt + 256])
        got = got[0:16] + got[16:32] + got[32:48]
        for g in range(SWEEPERS):
            ysend[g, :, 256 * nt : 256 * nt + 256] = got[4 * g : 4 * g + 4, :]

    c_rl.wait()
    lsend[...] = jnp.zeros_like(lsend)
    lsend[:, : PEERS * HS] = rl_v[...]

    c_nb.wait()
    c_fw.wait()
    c_sc.wait()
    c_de.wait()
    total = fw_v[0:1, :]
    for s in range(1, NB):
        total = total + fw_v[s : s + 1, :]
    total = total + 3.0 * sc_v[...]
    for v in range(2):
        extra = jnp.where(
            inst == 0, de_v[v : v + 1, :], jnp.where(inst == 1, de_v[2 + v : 3 + v, :], de_v[4 + v : 5 + v, :])
        )
        dsend[v : v + 1, :] = total + extra
    dsend[2:3, :] = sc_v[...]
    dsend[3:4, :] = sc_v[...]

    pl.semaphore_wait(barrier, partners)

    def taken_all(ref, sem):
        pltpu.make_async_copy(ref, ref, sem).wait()

    def list_copy(t):
        return pltpu.make_async_remote_copy(
            src_ref=lsend, dst_ref=lrx.at[t], send_sem=out_sem.at[0], recv_sem=list_sem.at[0],
            device_id={"cell": mirror(wrap(cell + OFFSETS[t])), "inst": inst}, device_id_type=MESH,
        )

    moves = ((dsend, drx), (nb_v, nb_r), (fw_v, fw_r))

    def move_copy(m):
        return pltpu.make_async_remote_copy(
            src_ref=moves[m][0], dst_ref=moves[m][1], send_sem=out_sem.at[6 + m], recv_sem=move_sem.at[m],
            device_id={"cell": me, "inst": inst}, device_id_type=MESH,
        )

    def move(m):
        @pl.when(swapped)
        def _():
            move_copy(m).start()

        @pl.when(jnp.logical_not(swapped))
        def _():
            pltpu.make_async_copy(*moves[m], move_sem.at[m]).start()

    def rest_copy(g, kind):
        if kind == 0:
            src, dst = ysend.at[g], rx.at[inst]
        else:
            src = ysend.at[g, :, pl.ds((0, cc - BLK)[kind - 1], BLK)]
            dst = rxe.at[kind - 1, inst]
        return pltpu.make_async_remote_copy(
            src_ref=src, dst_ref=dst, send_sem=out_sem.at[1 + min(kind, 1)], recv_sem=rest_sem.at[min(kind, 1)],
            device_id={"cell": mirror(wrap(cell + (0, 1, -1)[kind])), "inst": g}, device_id_type=MESH,
        )

    def halo_copy(k, t):
        return pltpu.make_async_remote_copy(
            src_ref=xsend.at[k, t // 4], dst_ref=halo.at[k, t], send_sem=out_sem.at[3], recv_sem=halo_sem.at[k],
            device_id={"cell": mirror(wrap(me - OFFSETS[t])), "inst": inst}, device_id_type=MESH,
        )

    def back_copy(g, kind):
        if kind == 0:
            src, dst = xf.at[g], gx.at[inst]
        else:
            src = xf.at[g, :, pl.ds((0, cc - BLK)[kind - 1], BLK)]
            dst = gxe.at[kind - 1, inst]
        return pltpu.make_async_remote_copy(
            src_ref=src, dst_ref=dst, send_sem=out_sem.at[4 + min(kind, 1)], recv_sem=back_sem.at[min(kind, 1)],
            device_id={"cell": wrap(me + (0, -1, 1)[kind]), "inst": g}, device_id_type=MESH,
        )

    sweeping = inst < SWEEPERS

    @pl.when(sweeping)
    def _():
        for t in (0, 5, 1, 4, 2, 3):
            if abs(OFFSETS[t]) == 2:
                here = mirror(wrap(cell + OFFSETS[t])) == cell

                @pl.when(here)
                def _():
                    pltpu.make_async_copy(lsend, lrx.at[t], list_sem.at[0]).start()

                @pl.when(jnp.logical_not(here))
                def _():
                    list_copy(t).start()
            else:
                list_copy(t).start()

    for kind in (1, 2):
        for g in range(SWEEPERS):
            rest_copy(g, kind).start()

    @pl.when(sweeping)
    def _():
        move(0)

    for g in range(SWEEPERS):
        local = (inst == g) & jnp.logical_not(swapped)

        @pl.when(jnp.logical_not(local))
        def _():
            rest_copy(g, 0).start()

        @pl.when(local)
        def _():
            pltpu.make_async_copy(ysend.at[g], rx.at[g], rest_sem.at[0]).start()

    @pl.when(sweeping)
    def _():
        move(1)
        move(2)

    row = lax.broadcasted_iota(jnp.int32, (ROWS, BLK), 0)
    row_n = 2 * (row // 4) + row % 2
    row_v = (row % 4) // 2
    live = [p for p in range(ROWS) if 2 * (p // 4) + p % 2 < HB_INST]
    for slot, p in enumerate(live):
        n, v = 2 * (p // 4) + p % 2, (p % 4) // 2
        value = jnp.zeros((ROWS, BLK), F32)
        for m in range(HB_INST):
            value = jnp.where((row_n == m) & (row_v == v), spectral_value(m - n), value)
        coef[slot] = value

    quarter = lax.broadcasted_iota(jnp.int32, (ROWS, BLK), 1) // HS

    def build(src, lane_tiles, first_tile):
        def one(m, _):
            lt, kt = m // 5, lax.rem(m, 5)
            s_lanes = pl.ds(pl.multiple_of(lt * BLK, BLK), BLK)
            d_lanes = pl.ds(pl.multiple_of((lt + first_tile) * BLK, BLK), BLK)
            kf = kt.astype(F32).astype(BF16)
            at = []
            def line(i):
                return jnp.broadcast_to(src[i : i + 1, s_lanes], (16, BLK)).astype(BF16)

            for s in range(NB):
                r = line(T_R + s)
                at.append(jnp.where(line(T_Q + s) == kf, r, jnp.full_like(r, -1.0)))
            hs = [line(T_H + s) for s in range(NB)]
            ls = [line(T_L + s) for s in range(NB)]
            for j in range(16):
                here = row16 + jnp.asarray(16.0 * j, BF16)
                h = jnp.zeros((16, BLK), BF16)
                low = jnp.zeros((16, BLK), BF16)
                for s in range(NB):
                    hit = at[s] == here
                    h = jnp.where(hit, hs[s], h)
                    low = jnp.where(hit, ls[s], low)
                k_rows = pl.ds(pl.multiple_of(kt * 256 + 16 * j, 16), 16)
                wh[k_rows, d_lanes] = h
                wl[k_rows, d_lanes] = low
            return 0

        lax.fori_loop(*(5 * tile for tile in lane_tiles), one, 0)

    tiles = (SEND + cc) // 256

    def keep(x_all):
        own_hi, own_lo = split2(x_all[:, SEND:])
        xh_v[0:16, :] = own_hi
        xh_v[16:32, :] = own_lo
        x_v[...] = x_all

    def local_part(which):
        for nt in which:
            lanes = pl.ds(256 * nt, 256)
            a = dot(xh_v[...], wh[0:cc, lanes])
            b = dot(xh_v[0:16, :], wl[0:cc, lanes])
            halves = []
            for e in range(2):
                part = pl.ds(256 * nt + 128 * e, 128)
                acc = jnp.zeros((ROWS, BLK), F32)
                for slot, p in enumerate(live):
                    acc = acc + coef[slot] * jnp.broadcast_to(x_v[p : p + 1, part], (ROWS, BLK))
                halves.append(acc)
            sx = jnp.concatenate(halves, axis=1)
            base_v[:, lanes] = r_v[:, lanes] - sg_v[:, lanes] * sx + (a[0:16] + a[16:32] + b)

    def halo_rows(k):
        taken_all(halo.at[k], halo_sem.at[k])
        first = halo[k, 0]
        for t in range(1, 4):
            first = jnp.where(quarter == t, halo[k, t], first)
        second = jnp.where(quarter == 0, halo[k, 4], jnp.where(quarter == 1, halo[k, 5], 0.0))
        hi, lo = split2(jnp.concatenate([first, second], axis=1))
        return jnp.concatenate([hi, lo], axis=0)

    def with_halo(rows, lanes):
        a = dot(rows, wh[cc : cc + 256, lanes])
        b = dot(rows[0:16], wl[cc : cc + 256, lanes])
        return (base_v[:, lanes] + (a[0:16] + a[16:32] + b)) * di_v[:, lanes]

    def send_halo(k, x_send):
        xsend[k, 0] = x_send[:, 0:BLK]
        xsend[k, 1] = x_send[:, BLK:SEND]
        for t in (0, 5, 1, 4, 2, 3):
            halo_copy(k, t).start()

    @pl.when(sweeping)
    def _():
        def own_table():
            taken_all(nb_r, move_sem.at[1])
            taken_all(fw_r, move_sem.at[2])
            ids = [jnp.broadcast_to(nb_r[s : s + 1, :], (8, cc)) for s in range(NB)]
            face = [jnp.broadcast_to(fw_r[s : s + 1, :], (8, cc)) for s in range(NB)]
            for s in range(NB):
                for o in range(s + 1, NB):
                    same = ids[s] == ids[o]
                    face[s] = face[s] + jnp.where(same, face[o], 0.0)
                    ids[o] = jnp.where(same, 2047, ids[o])
            for s in range(NB):
                table[T_Q + s : T_Q + s + 1, :] = lax.shift_right_logical(ids[s], 8).astype(F32)[0:1]
                table[T_R + s : T_R + s + 1, :] = (ids[s] & 255).astype(F32)[0:1]
                hi = face[s].astype(BF16).astype(F32)
                table[T_H + s : T_H + s + 1, :] = hi[0:1]
                table[T_L + s : T_L + s + 1, :] = (face[s] - hi).astype(BF16).astype(F32)[0:1]

        @pl.when(jnp.logical_not(swapped))
        def _():
            own_table()
            build(table, (0, EARLY), SEND // BLK)

        taken_all(lrx, list_sem.at[0])
        lane_slot = lax.broadcasted_iota(jnp.int32, (1, SEND), 1) // HS
        wanted = jnp.full((1, SEND), 4096, jnp.int32)
        for t in range(PEERS):
            wanted = jnp.where(lane_slot == t, lrx[t], wanted)
        for kt in range(cc // 256):
            rows256 = lax.broadcasted_iota(jnp.int32, (256, SEND), 0) + 256 * kt
            sel[256 * kt : 256 * kt + 256, :] = jnp.where(rows256 == wanted, 1.0, 0.0).astype(BF16)
        taken_all(drx, move_sem.at[0])
        late = dot(jnp.concatenate(split3(jnp.concatenate([drx[...], drx[...]], axis=0)), axis=0), sel[...])
        late = late[0:8] + late[8:16] + late[16:24]

        def by_variable(x, width):
            second = lax.rem(lax.broadcasted_iota(jnp.int32, (ROWS, width), 0), 4) >= 2
            return jnp.where(second, jnp.broadcast_to(x[1:2], (ROWS, width)), jnp.broadcast_to(x[0:1], (ROWS, width)))

        used = lane_slot < PEERS
        sg_v[:, 0:SEND] = jnp.broadcast_to(late[2:3], (ROWS, SEND))
        di_v[:, 0:SEND] = 1.0 / jnp.where(used, by_variable(late, SEND), 1.0)
        sg_v[:, SEND:] = jnp.broadcast_to(drx[2:3, :], (ROWS, cc))
        di_v[:, SEND:] = 1.0 / by_variable(drx[...], cc)
        taken_all(rxe, rest_sem.at[1])
        taken_all(rx, rest_sem.at[0])
        lane = lax.broadcasted_iota(jnp.int32, (ROWS, BLK), 1)
        mine = jnp.concatenate([rx[src] for src in range(n_inst)], axis=0)
        low = jnp.concatenate([rxe[0, src] for src in range(n_inst)], axis=0)
        high = jnp.concatenate([rxe[1, src] for src in range(n_inst)], axis=0)
        edge = handed * CB
        rest = jnp.concatenate(
            [
                jnp.where(lane < edge, low, mine[:, 0:BLK]),
                mine[:, BLK : cc - BLK],
                jnp.where(lane >= BLK - edge, high, mine[:, cc - BLK :]),
            ],
            axis=1,
        )
        parts = dot(jnp.concatenate(split3(rest), axis=0), sel[...])
        r_send = parts[0:16] + parts[16:32] + parts[32:48]
        x_send = r_send * di_v[:, 0:SEND]
        send_halo(0, x_send)
        r_v[:, 0:SEND] = r_send
        r_v[:, SEND:] = rest
        keep(jnp.concatenate([x_send, rest * di_v[:, SEND:]], axis=1))

        @pl.when(swapped)
        def _():
            own_table()

        stable[...] = dot(table[...].astype(BF16), sel[...])
        build(stable, (0, SEND // BLK), 0)
        local_part((0,))

        def own_sweep(rows, x_send):
            local_part(range(1, tiles))
            parts = [x_send]
            for nt in range(cc // 256):
                parts.append(with_halo(rows, pl.ds(SEND + 256 * nt, 256)))
            keep(jnp.concatenate(parts, axis=1))
            local_part((0,))

        rows = halo_rows(0)
        x_send = with_halo(rows, pl.ds(0, SEND))
        send_halo(1, x_send)
        build(table, (jnp.where(swapped, 0, EARLY), cc // BLK), SEND // BLK)
        own_sweep(rows, x_send)

        def sweep(k, _):
            rows = halo_rows(k)
            x_send = with_halo(rows, pl.ds(0, SEND))
            send_halo(k + 1, x_send)
            own_sweep(rows, x_send)
            return 0

        lax.fori_loop(1, ITERS - 1, sweep, 0)
        local_part(range(1, tiles))
        rows = halo_rows(ITERS - 1)
        for nt in (0, cc // 256 - 1, *range(1, cc // 256 - 1)):
            out = with_halo(rows, pl.ds(SEND + 256 * nt, 256))
            for g in range(n_inst):
                xf[g, :, 256 * nt : 256 * nt + 256] = out[4 * g : 4 * g + 4, :]
            if nt == cc // 256 - 1:
                for kind in (1, 2):
                    for g in range(n_inst):
                        back_copy(g, kind).start()
        for g in range(n_inst):
            local = (inst == g) & jnp.logical_not(swapped)

            @pl.when(jnp.logical_not(local))
            def _():
                back_copy(g, 0).start()

            if g < SWEEPERS:
                @pl.when(local)
                def _():
                    pltpu.make_async_copy(xf.at[g], gx.at[g], back_sem.at[0]).start()

    def permute_back(step, _):
        for u in range(2):
            permutation_tile(pos_v, perm_t, step * 2 + u)
        return 0

    lax.fori_loop(0, cc // BLK // 2, permute_back, 0)
    taken_all(gxe, back_sem.at[1])
    taken_all(gx, back_sem.at[0])
    lane4 = lax.broadcasted_iota(jnp.int32, (4, BLK), 1)
    edge = handed * CB
    placed = []
    for src in range(SWEEPERS):
        own = gx[src]
        first = jnp.where(lane4 < edge, gxe[0, src], own[:, 0:BLK])
        last = jnp.where(lane4 >= BLK - edge, gxe[1, src], own[:, cc - BLK :])
        coarse_o[src] = own
        placed.append(jnp.concatenate([first, own[:, BLK : cc - BLK], last], axis=1))
    terms = jnp.concatenate(split3(jnp.concatenate(placed + placed[2:], axis=0)), axis=0)
    for nt in range(cc // 256):
        got = dot(terms, perm_t[:, 256 * nt : 256 * nt + 256])
        got = got[0:16] + got[16:32] + got[32:48]
        for g in range(SWEEPERS):
            blocks_o[g, :, 256 * nt : 256 * nt + 256] = got[4 * g : 4 * g + 4, :]

    taken_all(ysend.at[:, :, 0:256], out_sem.at[2])

    @pl.when(sweeping & jnp.logical_not(swapped))
    def _():
        taken_all(ysend.at[0 : SWEEPERS - 1], out_sem.at[1])
        taken_all(xf.at[0 : n_inst - 1], out_sem.at[4])

    @pl.when(jnp.logical_not(sweeping) | swapped)
    def _():
        taken_all(ysend, out_sem.at[1])

    @pl.when(sweeping & swapped)
    def _():
        taken_all(xf, out_sem.at[4])
        for m in range(3):
            taken_all(moves[m][1], out_sem.at[6 + m])

    @pl.when(sweeping)
    def _():
        at_home = (mirror(wrap(cell + 2)) == cell) | (mirror(wrap(cell - 2)) == cell)

        @pl.when(at_home)
        def _():
            taken_all(lrx.at[0 : PEERS - 1], out_sem.at[0])

        @pl.when(jnp.logical_not(at_home))
        def _():
            taken_all(lrx, out_sem.at[0])

        taken_all(halo, out_sem.at[3])
        taken_all(xf.at[:, :, 0:256], out_sem.at[5])


def prolong(fm, coarse, blocks_x, fine_o, coarse_o):
    for v in range(VARS):
        coarse_o[v] = coarse[v // 2, 2 * (v % 2) : 2 * (v % 2) + 2, :]
    for tile in range(blocks_x.shape[2] // BLK):
        lanes = pl.ds(tile * BLK, BLK)
        for half in range(2):
            maps = [
                jnp.broadcast_to(fm[tile * 8 + 4 * half + e : tile * 8 + 4 * half + e + 1, :], (2, BLK)) + (4 * half + e) * CB
                for e in range(4)
            ]
            index = jnp.concatenate(maps, axis=0)
            rows = pl.ds(16 * tile + 8 * half, 8)
            for v in range(VARS):
                x = blocks_x[v // 2, 2 * (v % 2) : 2 * (v % 2) + 2, lanes]
                x = jnp.concatenate([x, x, x, x], axis=0)
                fine_o[v, rows, :] = jnp.take_along_axis(x, index, axis=1, mode="promise_in_bounds")


def body(n_cell, fine_residual, fine_map, routes, receive_lists, neighbours, face_weights, spectral_coef, diag_extra):
    inst_dev, var_count, fine_dev = fine_residual.shape
    blocks = fine_dev // BLK
    cc = blocks * CB
    lanes = SEND + cc
    vmem = pltpu.VMEM
    dma = pltpu.SemaphoreType.DMA
    any_spec = pl.BlockSpec(memory_space=pl.ANY)
    out_spec = pl.BlockSpec(memory_space=pltpu.VMEM)
    fine_rows = fine_residual.reshape(inst_dev, var_count, blocks, BLK).transpose(1, 2, 0, 3)
    fine_rows = fine_rows.reshape(var_count, blocks * inst_dev, BLK)
    cells_map = fine_map.reshape(blocks, BLK)
    coarse, in_blocks = pl.pallas_call(
        functools.partial(kernel, n_cell),
        out_shape=(
            pltpu.VMEM((SWEEPERS, 4, cc), F32),
            pltpu.VMEM((SWEEPERS, 4, cc), F32),
        ),
        in_specs=[any_spec] * 8,
        out_specs=(out_spec, out_spec),
        scratch_shapes=[
            vmem(fine_rows.shape, F32),
            vmem((blocks, BLK), jnp.int32),
            pltpu.SMEM((1, blocks), jnp.int32),
            vmem((1, PEERS * HS), jnp.int32),
            vmem((NB, cc), jnp.int32),
            vmem((NB, cc), F32),
            vmem((1, cc), F32),
            vmem((VARS, cc), F32),
            vmem((8, BLK), jnp.int32),
            vmem((8, BLK), jnp.int32),
            vmem((cc, cc), BF16),
            vmem((cc, cc), BF16),
            vmem((SWEEPERS, 4, cc), F32),
            vmem((SWEEPERS, 4, cc), F32),
            vmem((4, 4, cc), F32),
            vmem((2, 4, 4, BLK), F32),
            vmem((1, SEND), jnp.int32),
            vmem((PEERS, 1, SEND), jnp.int32),
            vmem((4, cc), F32),
            vmem((4, cc), F32),
            vmem((NB, cc), jnp.int32),
            vmem((NB, cc), F32),
            vmem((T_END, cc), F32),
            vmem((T_END, SEND), F32),
            vmem((cc, SEND), BF16),
            vmem((cc + 256, lanes), BF16),
            vmem((cc + 256, lanes), BF16),
            vmem((2 * HB_INST, ROWS, BLK), F32),
            vmem((ROWS, lanes), F32),
            vmem((ROWS, lanes), F32),
            vmem((ROWS, lanes), F32),
            vmem((ROWS, lanes), F32),
            vmem((ROWS, lanes), F32),
            vmem((2 * ROWS, cc), BF16),
            vmem((ITERS, 2, ROWS, BLK), F32),
            vmem((ITERS, PEERS, ROWS, BLK), F32),
            vmem((4, 4, cc), F32),
            vmem((SWEEPERS, 4, cc), F32),
            vmem((2, SWEEPERS, 4, BLK), F32),
            dma((8,)),
            dma((9,)),
            dma((1,)),
            dma((3,)),
            dma((2,)),
            dma((ITERS,)),
            dma((2,)),
        ],
        compiler_params=pltpu.CompilerParams(collective_id=0, has_side_effects=True),
        name="multigrid",
    )(
        fine_rows,
        cells_map,
        routes,
        receive_lists,
        neighbours,
        face_weights,
        spectral_coef.reshape(1, cc),
        diag_extra,
    )
    fine, coarse = pl.pallas_call(
        prolong,
        out_shape=(
            jax.ShapeDtypeStruct(fine_rows.shape, F32),
            jax.ShapeDtypeStruct((var_count, inst_dev, cc), F32),
        ),
        in_specs=[out_spec] * 3,
        out_specs=(out_spec, out_spec),
        compiler_params=pltpu.CompilerParams(vmem_limit_bytes=8 << 20),
        name="prolong",
    )(
        cells_map,
        pltpu.with_memory_space_constraint(coarse, pltpu.VMEM),
        pltpu.with_memory_space_constraint(in_blocks, pltpu.VMEM),
    )
    fine = fine.reshape(var_count, blocks, inst_dev, BLK).transpose(2, 0, 1, 3).reshape(inst_dev, var_count, fine_dev)
    return fine, coarse.transpose(1, 0, 2)


def solution(mesh):
    in_specs = (
        P("inst", None, "cell"),
        P("cell"),
        P("cell", None),
        P("cell", None),
        P(None, "cell"),
        P(None, "cell"),
        P("cell"),
        P(None, "cell"),
    )
    out_specs = (P("inst", None, "cell"), P("inst", None, "cell"))
    return jax.shard_map(
        functools.partial(body, mesh.shape["cell"]), mesh=mesh, in_specs=in_specs, out_specs=out_specs, check_vma=False
    )
```
